32 devices in a mesh: rep: 1 (over z), dp: 4 (over y), sp: 8 (over x, core).
Axes of the slice: x: 4, y: 4, z: 1, core: 2. Of those that a mesh axis runs over, the one named last changes fastest.
The devices are a block of a 4x4x8 slice.
Arguments:
- hidden: bfloat16 [32, 3584], P(('rep', 'dp'))
- w_query: bfloat16 [3584, 4096], replicated
- w_key: bfloat16 [3584, 2048], replicated
- w_value: bfloat16 [3584, 2048], replicated
- w_out: bfloat16 [4096, 3584], P('sp')
- k_cache: bfloat16 [32, 2048, 8, 256], P(('rep', 'dp'), 'sp')
- v_cache: bfloat16 [32, 2048, 8, 256], P(('rep', 'dp'), 'sp')
- write_pos: int32 [32], P(('rep', 'dp'))
- valid_len: int32 [32], P(('rep', 'dp'))
Outputs:
- output 1: bfloat16 [32, 3584], P(('rep', 'dp'))
- output 2: bfloat16 [32, 2048, 8, 256], P(('rep', 'dp'), 'sp')
- output 3: bfloat16 [32, 2048, 8, 256], P(('rep', 'dp'), 'sp')
All inputs are finite; a program needn't handle non-finite values.
Results may differ from the reference program's by a relative error of at most 0.00646443.
Values are sent between devices in bfloat16 or wider.
A program may use at most 768 MiB of HBM per device.

```python
import jax
import jax.numpy as jnp
from jax import lax

MODEL_DIM = 3584
NUM_HEADS = 16
KV_HEADS = 8
HEAD_DIM = 256
BATCH_SIZE = 32
CACHE_LEN = 2048
SEGMENTS = 32


def draw_lengths(rng_key):
    keys = jax.random.split(rng_key, 3)
    shortest = CACHE_LEN // 4
    write_pos = jax.random.randint(keys[0], (BATCH_SIZE,), shortest - 1, CACHE_LEN, jnp.int32)
    long_row = jax.random.randint(keys[1], (), 0, BATCH_SIZE, jnp.int32)
    short_row = (long_row + 1 + jax.random.randint(keys[2], (), 0, BATCH_SIZE - 1, jnp.int32)) % BATCH_SIZE
    row_ids = jnp.arange(BATCH_SIZE, dtype=jnp.int32)
    write_pos = jnp.where(row_ids == long_row, CACHE_LEN - 1, write_pos)
    write_pos = jnp.where(row_ids == short_row, shortest - 1, write_pos)
    return write_pos, write_pos + 1


def setup_inputs(seed: int = 0, part: int = 0) -> dict:
    root = jax.random.key(seed)
    shared = jax.random.split(root, 4)
    own = jax.random.split(jax.random.fold_in(root, part), 8)
    seg_len = CACHE_LEN // SEGMENTS
    proj_width = NUM_HEADS * HEAD_DIM
    kv_width = KV_HEADS * HEAD_DIM
    w_query = (jax.random.normal(shared[0], (MODEL_DIM, proj_width), jnp.float32) * MODEL_DIM ** -0.5).astype(jnp.bfloat16)
    w_key = (jax.random.normal(shared[1], (MODEL_DIM, kv_width), jnp.float32) * MODEL_DIM ** -0.5).astype(jnp.bfloat16)
    w_value = (jax.random.normal(shared[2], (MODEL_DIM, kv_width), jnp.float32) * MODEL_DIM ** -0.5).astype(jnp.bfloat16)
    w_out = (jax.random.normal(shared[3], (proj_width, MODEL_DIM), jnp.float32) * proj_width ** -0.5).astype(jnp.bfloat16)
    hidden = jax.random.normal(own[0], (BATCH_SIZE, MODEL_DIM), jnp.float32).astype(jnp.bfloat16)
    cache_shape = (BATCH_SIZE, SEGMENTS, seg_len, KV_HEADS, HEAD_DIM)
    seg_shape = (BATCH_SIZE, SEGMENTS, 1, KV_HEADS, HEAD_DIM)
    flat_shape = (BATCH_SIZE, CACHE_LEN, KV_HEADS, HEAD_DIM)
    k_cache = (jax.random.normal(own[1], cache_shape, jnp.float32) + jax.random.normal(own[2], seg_shape, jnp.float32)).reshape(flat_shape).astype(jnp.bfloat16)
    v_cache = (jax.random.normal(own[3], cache_shape, jnp.float32) + jax.random.normal(own[4], seg_shape, jnp.float32)).reshape(flat_shape).astype(jnp.bfloat16)
    write_pos, valid_len = draw_lengths(own[5])
    return {'hidden': hidden, 'w_query': w_query, 'w_key': w_key, 'w_value': w_value, 'w_out': w_out, 'k_cache': k_cache, 'v_cache': v_cache, 'write_pos': write_pos, 'valid_len': valid_len}


def reference(hidden, w_query, w_key, w_value, w_out, k_cache, v_cache, write_pos, valid_len):
    group_size = NUM_HEADS // KV_HEADS
    query = jnp.dot(hidden, w_query, preferred_element_type=jnp.float32).astype(jnp.bfloat16)
    query = query.reshape(BATCH_SIZE, KV_HEADS, group_size, HEAD_DIM)
    key_new = jnp.dot(hidden, w_key, preferred_element_type=jnp.float32).astype(jnp.bfloat16)
    value_new = jnp.dot(hidden, w_value, preferred_element_type=jnp.float32).astype(jnp.bfloat16)
    positions = jnp.arange(CACHE_LEN, dtype=jnp.int32)
    at_pos = (positions[None, :] == write_pos[:, None])[:, :, None, None]
    k_next = jnp.where(at_pos, key_new.reshape(BATCH_SIZE, 1, KV_HEADS, HEAD_DIM), k_cache)
    v_next = jnp.where(at_pos, value_new.reshape(BATCH_SIZE, 1, KV_HEADS, HEAD_DIM), v_cache)

    def one_row(row_args):
        q_row, k_row, v_row, length = row_args
        scores = jnp.einsum('kgd,skd->kgs', q_row.astype(jnp.float32), k_row.astype(jnp.float32)) * HEAD_DIM ** -0.5
        scores = jnp.where(positions < length, scores, -jnp.inf)
        row_max = jnp.max(scores, axis=-1, keepdims=True)
        weights = jnp.exp(scores - row_max)
        total = jnp.sum(weights, axis=-1, keepdims=True)
        return jnp.einsum('kgs,skd->kgd', weights, v_row.astype(jnp.float32)) / total

    attention = lax.map(one_row, (query, k_next, v_next, valid_len))
    attention = attention.reshape(BATCH_SIZE, NUM_HEADS * HEAD_DIM).astype(jnp.bfloat16)
    attn_out = jnp.dot(attention, w_out, preferred_element_type=jnp.float32).astype(jnp.bfloat16)
    return (attn_out, k_next, v_next)
```

```python
import functools

import jax
import jax.numpy as jnp
from jax import lax
from jax.experimental import pallas as pl
from jax.experimental.pallas import tpu as pltpu
from jax.sharding import PartitionSpec as P

F32 = jnp.float32
BF16 = jnp.bfloat16
FLOOR = float(jnp.finfo(jnp.float32).min)
MESH = pl.DeviceIdType.MESH
W_CHUNKS = 4
TILE = 32
MIB = 1 << 20


def _peer(me, off, n):
    return lax.rem(me + off, n)


def _greet(me, n):
    barrier = pltpu.get_barrier_semaphore()
    for off in range(1, n):
        pl.semaphore_signal(barrier, inc=1, device_id={'sp': _peer(me, off, n)}, device_id_type=MESH)
    return barrier


def _exchange(me, n, src, dst, ssem, rsem):
    return [
        pltpu.make_async_remote_copy(
            src_ref=src(_peer(me, off, n)), dst_ref=dst(off), send_sem=ssem.at[off - 1], recv_sem=rsem.at[off - 1],
            device_id={'sp': _peer(me, off, n)}, device_id_type=MESH)
        for off in range(1, n)
    ]


def _rows(i, count):
    return pl.ds(pl.multiple_of(i * count, count), count)


def _project(n, hid_ref, wq_ref, wk_ref, wv_ref, kc_ref, vc_ref,
             all_ref, k_ref, v_ref,
             hid, wqb, wkb, wvb, mine, got,
             hsem, wsem, ksem, vsem, s1, r1):
    me = lax.axis_index('sp')
    rows = hid.shape[0]
    depth, qw = wqb.shape
    dim = wkb.shape[1]
    ck = depth // W_CHUNKS
    hcopy = pltpu.make_async_copy(hid_ref, hid, hsem)
    hcopy.start()

    def w_copies(c):
        rs = pl.ds(c * ck, ck)
        return [
            pltpu.make_async_copy(wq_ref.at[rs, _rows(me, qw)], wqb.at[rs], wsem.at[c, 0]),
            pltpu.make_async_copy(wk_ref.at[rs, _rows(me, dim)], wkb.at[rs], wsem.at[c, 1]),
            pltpu.make_async_copy(wv_ref.at[rs, _rows(me, dim)], wvb.at[rs], wsem.at[c, 2]),
        ]

    def kv_copies(b):
        return [
            pltpu.make_async_copy(kc_ref.at[b], k_ref.at[b], ksem.at[b]),
            pltpu.make_async_copy(vc_ref.at[b], v_ref.at[b], vsem.at[b]),
        ]

    for c in range(W_CHUNKS):
        for cp in w_copies(c):
            cp.start()
    barrier = _greet(me, n)
    hcopy.wait()
    acc_q = jnp.zeros((rows, qw), F32)
    acc_k = jnp.zeros((rows, dim), F32)
    acc_v = jnp.zeros((rows, dim), F32)
    for c in range(W_CHUNKS):
        for cp in w_copies(c):
            cp.wait()
        for b in range(c * rows // W_CHUNKS, (c + 1) * rows // W_CHUNKS):
            for cp in kv_copies(b):
                cp.start()
        rs = pl.ds(c * ck, ck)
        h = hid[:, rs]
        acc_q += jnp.dot(h, wqb[rs], preferred_element_type=F32)
        acc_k += jnp.dot(h, wkb[rs], preferred_element_type=F32)
        acc_v += jnp.dot(h, wvb[rs], preferred_element_type=F32)
    mine[:, :qw] = acc_q.astype(BF16)
    mine[:, qw:qw + dim] = acc_k.astype(BF16)
    mine[:, qw + dim:] = acc_v.astype(BF16)
    pl.semaphore_wait(barrier, n - 1)
    x1 = _exchange(me, n, lambda peer: mine, lambda off: got.at[off - 1], s1, r1)
    for cp in x1:
        cp.start()

    def spread(src, value):
        value = value.astype(F32)
        for c in range(value.shape[1] // 128):
            all_ref[c, _rows(src, rows), :] = value[:, c * 128:(c + 1) * 128]

    spread(me, mine[...])
    for off in range(1, n):
        x1[off - 1].wait()
        spread(_peer(me, n - off, n), got[off - 1])
    for b in range(rows):
        for cp in kv_copies(b):
            cp.wait()


def _attend(n, wp_ref, vl_ref, all_ref, ki_ref, vi_ref, k_ref, v_ref, ko_ref, vo_ref, acc_ref, st_ref, ksem, vsem):
    del ki_ref, vi_ref
    me = lax.axis_index('sp')
    rows, seq, heads, dim = ko_ref.shape
    width = seq * heads
    ntile = seq // TILE
    w = TILE * heads
    scale = dim ** -0.5
    lane = lax.broadcasted_iota(jnp.int32, (heads, 128), 1)
    blocks = dim // 128

    def new_rows(b, first):
        return jnp.concatenate([all_ref[first + c, pl.ds(b, n, stride=rows), :] for c in range(blocks)], axis=1)

    def copies(b):
        return [
            pltpu.make_async_copy(k_ref.at[b], ko_ref.at[b], ksem.at[b]),
            pltpu.make_async_copy(v_ref.at[b], vo_ref.at[b], vsem.at[b]),
        ]

    for b in range(rows):
        at = wp_ref[b] - me * seq

        @pl.when((at >= 0) & (at < seq))
        def _():
            k_ref[b, at] = new_rows(b, 2 * blocks).astype(BF16)
            v_ref[b, at] = new_rows(b, 3 * blocks).astype(BF16)

    for b in range(rows):
        for cp in copies(b):
            cp.start()
    col = lax.broadcasted_iota(jnp.int32, (2 * heads, width), 1)
    row = lax.broadcasted_iota(jnp.int32, (2 * heads, width), 0)
    same = (col % heads) == (row % heads)
    colpos = col // heads

    def step(b, carry):
        q = jnp.concatenate([new_rows(b, 0), new_rows(b, blocks)], axis=0).astype(BF16)
        vl = vl_ref[b] - me * seq
        scores = []
        for t in range(ntile):
            kt = k_ref[b, pl.ds(t * TILE, TILE)].reshape(w, dim)
            scores.append(lax.dot_general(q, kt, (((1,), (1,)), ((), ())), preferred_element_type=F32))
        s = jnp.concatenate(scores, axis=1) * scale
        s = jnp.where(same & (colpos < vl), s, -jnp.inf)
        m = jnp.maximum(jnp.max(s, axis=-1, keepdims=True), FLOOR)
        p = jnp.exp(s - m)
        l = jnp.sum(p, axis=-1, keepdims=True)
        pb = p.astype(BF16)
        acc = jnp.zeros((2 * heads, dim), F32)
        for t in range(ntile):
            vt = v_ref[b, pl.ds(t * TILE, TILE)].reshape(w, dim)
            acc += jnp.dot(pb[:, t * w:(t + 1) * w], vt, preferred_element_type=F32)
        for c in range(blocks):
            piece = acc[:, c * 128:(c + 1) * 128]
            acc_ref[c, pl.ds(b, heads, stride=2 * rows), :] = piece[:heads]
            acc_ref[c, pl.ds(b + rows, heads, stride=2 * rows), :] = piece[heads:]
        st = jnp.where(lane == 0, m[:heads], jnp.where(lane == 1, l[:heads], jnp.where(lane == 2, m[heads:], l[heads:])))
        st_ref[pl.ds(b, heads, stride=rows), :] = st
        return carry

    lax.fori_loop(0, rows, step, 0)
    for b in range(rows):
        for cp in copies(b):
            cp.wait()


def _finish(n, sacc, st_ref, wo_ref, out_ref, w_ref, racc, rst, part, recv, red, gath,
            wsem, s2, r2, s3, r3, s4, r4, s5, r5):
    me = lax.axis_index('sp')
    rows, model = out_ref.shape
    blocks = sacc.shape[0]
    cols = part.shape[1] // n
    wcopy = pltpu.make_async_copy(wo_ref, w_ref, wsem)
    wcopy.start()
    barrier = _greet(me, n)
    pl.semaphore_wait(barrier, n - 1)
    x2 = _exchange(me, n, lambda peer: sacc.at[:, _rows(peer, 2 * rows)], lambda off: racc.at[off - 1], s2, r2)
    x3 = _exchange(me, n, lambda peer: st_ref.at[_rows(peer, rows)], lambda off: rst.at[off - 1], s3, r3)
    for a, b in zip(x2, x3):
        b.start()
        a.start()
    racc[n - 1] = sacc[:, _rows(me, 2 * rows), :]
    sts = [st_ref[_rows(me, rows), :]]
    for off in range(1, n):
        x3[off - 1].wait()
        sts.append(rst[off - 1])
    order = [n - 1] + list(range(n - 1))
    scales, totals = [], []
    for j in range(2):
        ms = [st[:, 2 * j:2 * j + 1] for st in sts]
        top = functools.reduce(jnp.maximum, ms)
        scales.append([jnp.exp(m - top) for m in ms])
        totals.append(functools.reduce(jnp.add, [st[:, 2 * j + 1:2 * j + 2] * e for st, e in zip(sts, scales[j])]))
    for cp in x2:
        cp.wait()
    pieces = []
    for j in range(2):
        for c in range(blocks):
            num = functools.reduce(jnp.add, [racc[i, c, j * rows:(j + 1) * rows, :] * e for i, e in zip(order, scales[j])])
            pieces.append((num / totals[j]).astype(BF16))
    o = jnp.concatenate(pieces, axis=1)
    wcopy.wait()
    part[:, :model] = jnp.dot(o, w_ref[...], preferred_element_type=F32)
    part[:, model:] = jnp.zeros((rows, part.shape[1] - model), F32)
    rs = _exchange(me, n, lambda peer: part.at[:, _rows(peer, cols)], lambda off: recv.at[off - 1], s4, r4)
    for cp in rs:
        cp.start()
    total = part[:, _rows(me, cols)]
    for off in range(1, n):
        rs[off - 1].wait()
        total += recv[off - 1]
    red[...] = total.astype(BF16)
    ag = _exchange(me, n, lambda peer: red, lambda off: gath.at[:, _rows(me, cols)], s5, r5)
    for cp in ag:
        cp.start()
    for cp in ag:
        cp.wait()
    gath[:, _rows(me, cols)] = red[...]
    out_ref[...] = gath[:, :model]


def solution(mesh):
    row_spec = P(('rep', 'dp'), None)
    cache_spec = P(('rep', 'dp'), 'sp', None, None)
    len_spec = P(('rep', 'dp'))
    n = mesh.shape['sp']
    vmem = pl.BlockSpec(memory_space=pltpu.VMEM)
    smem = pl.BlockSpec(memory_space=pltpu.SMEM)
    hbm = pl.BlockSpec(memory_space=pltpu.HBM)
    dma = pltpu.SemaphoreType.DMA

    def in_hbm(x):
        return pltpu.with_memory_space_constraint(x, pltpu.HBM)

    def local_step(hidden, w_query, w_key, w_value, w_out, k_cache, v_cache, write_pos, valid_len):
        rows, seq, heads, dim = k_cache.shape
        depth = hidden.shape[1]
        model = w_out.shape[1]
        qw = w_query.shape[1] // n
        lw = qw + 2 * dim
        blocks = dim // 128
        cache = pltpu.VMEM(k_cache.shape, BF16)
        proj, k_here, v_here = pl.pallas_call(
            functools.partial(_project, n),
            out_shape=(pltpu.VMEM((lw // 128, n * rows, 128), F32), cache, cache),
            in_specs=[hbm] * 6,
            out_specs=(vmem,) * 3,
            scratch_shapes=[
                pltpu.VMEM((rows, depth), BF16),
                pltpu.VMEM((depth, qw), BF16),
                pltpu.VMEM((depth, dim), BF16),
                pltpu.VMEM((depth, dim), BF16),
                pltpu.VMEM((rows, lw), BF16),
                pltpu.VMEM((n - 1, rows, lw), BF16),
                dma, dma((W_CHUNKS, 3)), dma((rows,)), dma((rows,)), dma((n - 1,)), dma((n - 1,)),
            ],
            compiler_params=pltpu.CompilerParams(collective_id=0, has_side_effects=True, vmem_limit_bytes=12 * MIB),
            cost_estimate=pl.CostEstimate(flops=10_000_000_000, bytes_accessed=28 * MIB, transcendentals=0),
            name='project',
        )(*[in_hbm(x) for x in (hidden, w_query, w_key, w_value, k_cache, v_cache)])
        _, _, k_next, v_next, acc, st = pl.pallas_call(
            functools.partial(_attend, n),
            out_shape=(
                cache, cache,
                jax.ShapeDtypeStruct(k_cache.shape, BF16),
                jax.ShapeDtypeStruct(v_cache.shape, BF16),
                pltpu.VMEM((blocks, heads * 2 * rows, 128), F32),
                pltpu.VMEM((heads * rows, 128), F32),
            ),
            in_specs=[smem, smem, vmem, vmem, vmem],
            out_specs=(vmem, vmem, hbm, hbm, vmem, vmem),
            scratch_shapes=[dma((rows,)), dma((rows,))],
            input_output_aliases={3: 0, 4: 1},
            compiler_params=pltpu.CompilerParams(vmem_limit_bytes=8 * MIB),
            cost_estimate=pl.CostEstimate(flops=5_000_000_000, bytes_accessed=16 * MIB, transcendentals=0),
            name='attend',
        )(write_pos, valid_len, proj, k_here, v_here)
        padded = -(-model // (128 * n)) * 128 * n
        attn = pl.pallas_call(
            functools.partial(_finish, n),
            out_shape=jax.ShapeDtypeStruct((rows, model), BF16),
            in_specs=[vmem, vmem, hbm],
            out_specs=vmem,
            scratch_shapes=[
                pltpu.VMEM(w_out.shape, BF16),
                pltpu.VMEM((n, blocks, 2 * rows, 128), F32),
                pltpu.VMEM((n - 1, rows, 128), F32),
                pltpu.VMEM((rows, padded), F32),
                pltpu.VMEM((n - 1, rows, padded // n), F32),
                pltpu.VMEM((rows, padded // n), BF16),
                pltpu.VMEM((rows, padded), BF16),
                dma,
            ] + [dma((n - 1,))] * 8,
            compiler_params=pltpu.CompilerParams(collective_id=1, has_side_effects=True, vmem_limit_bytes=8 * MIB),
            cost_estimate=pl.CostEstimate(flops=20_000_000_000, bytes_accessed=4 * MIB, transcendentals=0),
            name='finish',
        )(acc, st, in_hbm(w_out))
        return attn, k_next, v_next

    return jax.shard_map(
        local_step, mesh=mesh,
        in_specs=(row_spec, P(), P(), P(), P('sp', None), cache_spec, cache_spec, len_spec, len_spec),
        out_specs=(row_spec, cache_spec, cache_spec), check_vma=False)
```

```python
import functools

import jax
import jax.numpy as jnp
from jax import lax
from jax.experimental import pallas as pl
from jax.experimental.pallas import tpu as pltpu
from jax.sharding import PartitionSpec as P

F32 = jnp.float32
BF16 = jnp.bfloat16
FLOOR = float(jnp.finfo(jnp.float32).min)
MESH = pl.DeviceIdType.MESH
W_PARTS = (5, 4, 3, 2)
K_AFTER = (0, 0, 4, 16, 16)
EARLY = 5
TILE = 32
LAG = 2
MIB = 1 << 20


def _peer(me, off, n):
    return lax.rem(me + off, n)


def _greet(me, n):
    barrier = pltpu.get_barrier_semaphore()
    for off in range(1, n):
        pl.semaphore_signal(barrier, inc=1, device_id={'sp': _peer(me, off, n)}, device_id_type=MESH)
    return barrier


def _exchange(me, n, src, dst, ssem, rsem):
    def copy(off):
        peer = _peer(me, off, n)
        return pltpu.make_async_remote_copy(
            src_ref=src(peer), dst_ref=dst(off), send_sem=ssem.at[off - 1], recv_sem=rsem.at[off - 1],
            device_id={'sp': peer}, device_id_type=MESH)

    copies = [copy(off) for off in range(1, n)]
    for i in sorted(range(n - 1), key=lambda i: abs(i + 1 - n // 2)):
        copies[i].start()
    return copies


def _positions(heads, width, never):
    col = lax.broadcasted_iota(jnp.int32, (2 * heads, width), 1)
    row = lax.broadcasted_iota(jnp.int32, (2 * heads, width), 0)
    return jnp.where((col % heads) == (row % heads), col // heads, never)


def _rows(i, count):
    return pl.ds(pl.multiple_of(i * count, count), count)


def _project(n, hid_ref, wq_ref, wk_ref, wv_ref, kc_ref, vc_ref, wp_ref, vl_ref,
             s_ref, q_ref, end_ref, hit_ref, kn_ref, vn_ref, k_ref, v_ref,
             hid, wqb, wkb, wvb, acc, mine, got, full, wp, vl,
             hsem, wsem, ksem, vsem, psem, s1, r1):
    me = lax.axis_index('sp')
    rows, seq, heads, dim = k_ref.shape
    depth, qw = wqb.shape
    blocks = dim // 128
    w = TILE * heads
    small = [
        pltpu.make_async_copy(hid_ref, hid, hsem),
        pltpu.make_async_copy(wp_ref, wp, psem.at[0]),
        pltpu.make_async_copy(vl_ref, vl, psem.at[1]),
    ]
    for cp in small:
        cp.start()
    edges = [0]
    for part in W_PARTS:
        edges.append(edges[-1] + depth // dim * part // sum(W_PARTS) * dim)
    chunks = len(W_PARTS)

    def w_copies(c):
        rs = pl.ds(edges[c], edges[c + 1] - edges[c])
        return [
            pltpu.make_async_copy(wq_ref.at[rs, _rows(me, qw)], wqb.at[rs], wsem.at[c, 0]),
            pltpu.make_async_copy(wk_ref.at[rs, _rows(me, dim)], wkb.at[rs], wsem.at[c, 1]),
            pltpu.make_async_copy(wv_ref.at[rs, _rows(me, dim)], wvb.at[rs], wsem.at[c, 2]),
        ]

    k_copies = [pltpu.make_async_copy(kc_ref.at[b], k_ref.at[b], ksem.at[b]) for b in range(rows)]
    v_copies = [pltpu.make_async_copy(vc_ref.at[b], v_ref.at[b], vsem.at[b]) for b in range(rows)]
    queue = k_copies + v_copies
    for c in range(chunks):
        for cp in w_copies(c):
            cp.start()
    barrier = _greet(me, n)
    for cp in small:
        cp.wait()

    for c in range(chunks):
        for cp in w_copies(c):
            cp.wait()
        for cp in queue[len(queue) * K_AFTER[c] // 16:len(queue) * K_AFTER[c + 1] // 16]:
            cp.start()

        @pl.when(me >= 0)
        def _():
            ks = pl.ds(edges[c], edges[c + 1] - edges[c])
            parts = [jnp.dot(hid[:, ks], ref[ks, :], preferred_element_type=F32) for ref in (wqb, wkb, wvb)]
            total = jnp.concatenate(parts, axis=1)
            acc[...] = total if c == 0 else acc[...] + total

    mine[...] = acc[...].astype(BF16)
    pl.semaphore_wait(barrier, n - 1)
    x1 = _exchange(me, n, lambda peer: mine, lambda off: got.at[off - 1], s1, r1)

    def spread(src, value):
        value = value.astype(F32)
        for c in range(value.shape[1] // 128):
            full[c, _rows(src, rows), :] = value[:, c * 128:(c + 1) * 128]

    pos = lax.broadcasted_iota(jnp.int32, (1, seq), 1) + me * seq
    for b in range(rows):
        hit_ref[b:b + 1, :] = jnp.where(pos == wp[b], 1, 0)
    spread(me, mine[...])
    for off in range(1, n):
        x1[off - 1].wait()
        spread(_peer(me, n - off, n), got[off - 1])

    def of_row(b, first):
        return jnp.concatenate([full[first * blocks + c, pl.ds(b, n, stride=rows), :] for c in range(blocks)], axis=1)

    colpos = _positions(heads, w, 2 * seq * n)
    ntile = seq // TILE
    scale = dim ** -0.5

    for b in range(rows):
        q = jnp.concatenate([of_row(b, 0), of_row(b, 1)], axis=0).astype(BF16)
        kn = of_row(b, 2).astype(BF16)
        end = vl[b] - me * seq
        at = wp[b] - me * seq
        q_ref[b] = q
        kn_ref[b] = kn
        vn_ref[b] = of_row(b, 3).astype(BF16)
        end_ref[b:b + 1, :] = jnp.full((1, w), end, jnp.int32)
        if b >= EARLY:
            continue
        k_copies[b].wait()

        def times(kt):
            return lax.dot_general(q, kt, (((1,), (1,)), ((), ())), preferred_element_type=F32)

        fresh = times(jnp.concatenate([kn[None]] * TILE, axis=0).reshape(w, dim))
        for t in range(ntile):
            s = jnp.where(colpos == at - t * TILE, fresh, times(k_ref[b, pl.ds(t * TILE, TILE)].reshape(w, dim))) * scale
            s_ref[b, :, t * w:(t + 1) * w] = jnp.where(colpos < end - t * TILE, s, -jnp.inf)

    for cp in k_copies[EARLY:]:
        cp.wait()
    for cp in v_copies:
        cp.wait()


def _attend(n, s_ref, q_ref, end_ref, k_ref, v_ref, wo_ref, out_ref, w_ref, p_ref, xs, xr, part, recv, red, gath,
            wsem, s2, r2, s4, r4, s5, r5):
    me = lax.axis_index('sp')
    rows, seq, heads, dim = v_ref.shape
    model = out_ref.shape[1]
    cols = part.shape[1] // n
    blocks = dim // 128
    ntile = seq // TILE
    w = TILE * heads
    span = xs.shape[0] // heads
    wcopy = pltpu.make_async_copy(wo_ref, w_ref, wsem)
    wcopy.start()
    barrier = _greet(me, n)
    lane = lax.broadcasted_iota(jnp.int32, (heads, 128), 1)
    colpos = _positions(heads, w, 2 * seq * n)
    scale = dim ** -0.5

    def score(b):
        return [lax.dot_general(q_ref[b], k_ref[b, pl.ds(t * TILE, TILE)].reshape(w, dim), (((1,), (1,)), ((), ())),
                                preferred_element_type=F32) for t in range(ntile)]

    def soften(b, ss):
        if ss is None:
            ss = [s_ref[b, :, t * w:(t + 1) * w] for t in range(ntile)]
        else:
            end = end_ref[b:b + 1, :]
            ss = [jnp.where(colpos < end - t * TILE, s * scale, -jnp.inf) for t, s in enumerate(ss)]
        m = jnp.max(functools.reduce(jnp.maximum, ss), axis=-1, keepdims=True)
        m = jnp.maximum(m, FLOOR)
        ps = [jnp.exp(s - m) for s in ss]
        l = jnp.sum(functools.reduce(jnp.add, ps), axis=-1, keepdims=True)
        for t in range(ntile):
            p_ref[b, :, t * w:(t + 1) * w] = ps[t].astype(BF16)
        st = jnp.where(lane == 0, m[:heads], jnp.where(lane == 1, l[:heads], jnp.where(lane == 2, m[heads:], l[heads:])))
        xs[pl.ds(blocks * 2 * rows + b, heads, stride=span), :] = st

    def values(b):
        acc = functools.reduce(jnp.add, [
            functools.reduce(jnp.add, [
                jnp.dot(p_ref[b, :, t * w:(t + 1) * w], v_ref[b, pl.ds(t * TILE, TILE)].reshape(w, dim),
                        preferred_element_type=F32) for t in range(first, ntile, 2)]) for first in range(2)])
        for c in range(blocks):
            piece = acc[:, c * 128:(c + 1) * 128]
            xs[pl.ds(c * 2 * rows + b, heads, stride=span), :] = piece[:heads]
            xs[pl.ds(c * 2 * rows + rows + b, heads, stride=span), :] = piece[heads:]

    for i in range(rows + LAG):
        if i < rows:
            soften(i, score(i) if i >= EARLY else None)
        if i >= LAG:
            values(i - LAG)
    pl.semaphore_wait(barrier, n - 1)
    x2 = _exchange(me, n, lambda peer: xs.at[_rows(peer, span)], lambda off: xr.at[off - 1], s2, r2)
    xr[n - 1] = xs[_rows(me, span), :]
    for cp in x2:
        cp.wait()
    base = blocks * 2 * rows
    pieces = []
    sts = [xr[i, base:base + rows, :] for i in range(n)]
    for j in range(2):
        ms = [st[:, 2 * j:2 * j + 1] for st in sts]
        top = functools.reduce(jnp.maximum, ms)
        es = [jnp.exp(m - top) for m in ms]
        total = functools.reduce(jnp.add, [st[:, 2 * j + 1:2 * j + 2] * e for st, e in zip(sts, es)])
        for c in range(blocks):
            at = c * 2 * rows + j * rows
            num = functools.reduce(jnp.add, [xr[i, at:at + rows, :] * es[i] for i in range(n)])
            pieces.append((num / total).astype(BF16))
    o = jnp.concatenate(pieces, axis=1)
    wcopy.wait()

    part[:, :model] = jnp.dot(o, w_ref[...], preferred_element_type=F32)
    part[:, model:] = jnp.zeros((rows, part.shape[1] - model), F32)
    rs = _exchange(me, n, lambda peer: part.at[:, _rows(peer, cols)], lambda off: recv.at[off - 1], s4, r4)
    total = part[:, _rows(me, cols)]
    for off in range(1, n):
        rs[off - 1].wait()
        total += recv[off - 1]
    red[...] = total.astype(BF16)
    ag = _exchange(me, n, lambda peer: red, lambda off: gath.at[:, _rows(me, cols)], s5, r5)
    for cp in ag:
        cp.wait()
    gath[:, _rows(me, cols)] = red[...]
    out_ref[...] = gath[:, :model]


def _hand_over(attn_ref, k_ref, v_ref, out_ref):
    del k_ref, v_ref
    out_ref[...] = attn_ref[...]


def solution(mesh):
    row_spec = P(('rep', 'dp'), None)
    cache_spec = P(('rep', 'dp'), 'sp', None, None)
    len_spec = P(('rep', 'dp'))
    n = mesh.shape['sp']
    vmem = pl.BlockSpec(memory_space=pltpu.VMEM)
    hbm = pl.BlockSpec(memory_space=pltpu.HBM)
    dma = pltpu.SemaphoreType.DMA

    def in_hbm(x):
        return pltpu.with_memory_space_constraint(x, pltpu.HBM)

    def local_step(hidden, w_query, w_key, w_value, w_out, k_cache, v_cache, write_pos, valid_len):
        rows, seq, heads, dim = k_cache.shape
        depth = hidden.shape[1]
        model = w_out.shape[1]
        qw = w_query.shape[1] // n
        lw = qw + 2 * dim
        blocks = dim // 128
        cache = pltpu.VMEM(k_cache.shape, BF16)
        new = pltpu.VMEM((rows, heads, dim), BF16)
        scores, query, ends, hit, k_new, v_new, k_here, v_here = pl.pallas_call(
            functools.partial(_project, n),
            out_shape=(
                pltpu.VMEM((EARLY, 2 * heads, seq * heads), F32),
                pltpu.VMEM((rows, 2 * heads, dim), BF16),
                pltpu.VMEM((rows, TILE * heads), jnp.int32),
                pltpu.VMEM((rows, seq), jnp.int32),
                new, new, cache, cache,
            ),
            in_specs=[hbm] * 8,
            out_specs=(vmem,) * 8,
            scratch_shapes=[
                pltpu.VMEM((rows, depth), BF16),
                pltpu.VMEM((depth, qw), BF16),
                pltpu.VMEM((depth, dim), BF16),
                pltpu.VMEM((depth, dim), BF16),
                pltpu.VMEM((rows, lw), F32),
                pltpu.VMEM((rows, lw), BF16),
                pltpu.VMEM((n - 1, rows, lw), BF16),
                pltpu.VMEM((lw // 128, n * rows, 128), F32),
                pltpu.SMEM((rows,), jnp.int32),
                pltpu.SMEM((rows,), jnp.int32),
                dma, dma((len(W_PARTS), 3)), dma((rows,)), dma((rows,)), dma((2,)), dma((n - 1,)), dma((n - 1,)),
            ],
            compiler_params=pltpu.CompilerParams(collective_id=0, has_side_effects=True, vmem_limit_bytes=12 * MIB),
            cost_estimate=pl.CostEstimate(flops=10_000_000_000, bytes_accessed=28 * MIB, transcendentals=0),
            name='project',
        )(*[in_hbm(x) for x in (hidden, w_query, w_key, w_value, k_cache, v_cache, write_pos, valid_len)])
        at_pos = (hit != 0)[:, :, None, None]
        k_next = jnp.where(at_pos, k_new[:, None], k_here)
        v_next = jnp.where(at_pos, v_new[:, None], v_here)
        padded = -(-model // (128 * n)) * 128 * n
        span = 2 * rows * blocks + rows
        attn = pl.pallas_call(
            functools.partial(_attend, n),
            out_shape=jax.ShapeDtypeStruct((rows, model), BF16),
            in_specs=[vmem] * 5 + [hbm],
            out_specs=vmem,
            scratch_shapes=[
                pltpu.VMEM(w_out.shape, BF16),
                pltpu.VMEM((rows, 2 * heads, seq * heads), BF16),
                pltpu.VMEM((heads * span, 128), F32),
                pltpu.VMEM((n, span, 128), F32),
                pltpu.VMEM((rows, padded), F32),
                pltpu.VMEM((n - 1, rows, padded // n), F32),
                pltpu.VMEM((rows, padded // n), BF16),
                pltpu.VMEM((rows, padded), BF16),
                dma,
            ] + [dma((n - 1,))] * 6,
            compiler_params=pltpu.CompilerParams(collective_id=1, has_side_effects=True, vmem_limit_bytes=8 * MIB),
            cost_estimate=pl.CostEstimate(flops=20_000_000_000, bytes_accessed=4 * MIB, transcendentals=0),
            name='attend',
        )(scores, query, ends, k_next, v_next, in_hbm(w_out))
        attn = pl.pallas_call(
            _hand_over,
            out_shape=jax.ShapeDtypeStruct((rows, model), BF16),
            in_specs=[vmem] * 3,
            out_specs=vmem,
            compiler_params=pltpu.CompilerParams(vmem_limit_bytes=1 * MIB),
            name='hand_over',
        )(attn, k_next, v_next)
        return attn, k_next, v_next

    return jax.shard_map(
        local_step, mesh=mesh,
        in_specs=(row_spec, P(), P(), P(), P('sp', None), cache_spec, cache_spec, len_spec, len_spec),
        out_specs=(row_spec, cache_spec, cache_spec), check_vma=False)
```

```python
import functools

import jax
import jax.numpy as jnp
from jax import lax
from jax.experimental import pallas as pl
from jax.experimental.pallas import tpu as pltpu
from jax.sharding import PartitionSpec as P

F32 = jnp.float32
BF16 = jnp.bfloat16
FLOOR = float(jnp.finfo(jnp.float32).min)
MESH = pl.DeviceIdType.MESH
Q_PARTS = (6, 5, 3)
KV_PARTS = (8, 6)
K_PARTS = 4
K_FIRST = 2
V_PARTS = 2
EARLY = 6
TILE = 32
LAG = 2
MIB = 1 << 20


def _peer(me, off, n):
    return lax.rem(me + off, n)


def _greet(me, n):
    barrier = pltpu.get_barrier_semaphore()
    for off in range(1, n):
        pl.semaphore_signal(barrier, inc=1, device_id={'sp': _peer(me, off, n)}, device_id_type=MESH)
    return barrier


def _far_first(n):
    return sorted(range(1, n), key=lambda off: abs(off - n // 2))


def _exchange(me, n, src, dst, ssem, rsem):
    def copy(off):
        peer = _peer(me, off, n)
        return pltpu.make_async_remote_copy(
            src_ref=src(peer), dst_ref=dst(off), send_sem=ssem.at[off - 1], recv_sem=rsem.at[off - 1],
            device_id={'sp': peer}, device_id_type=MESH)

    copies = [copy(off) for off in range(1, n)]
    for off in _far_first(n):
        copies[off - 1].start()
    return copies


def _part(i, size, parts):
    return pl.ds(i * size // parts, size // parts)


def _positions(heads, width, never):
    col = lax.broadcasted_iota(jnp.int32, (2 * heads, width), 1)
    row = lax.broadcasted_iota(jnp.int32, (2 * heads, width), 0)
    return jnp.where((col % heads) == (row % heads), col // heads, never)


def _rows(i, count):
    return pl.ds(pl.multiple_of(i * count, count), count)


def _project(n, hid_ref, wq_ref, wk_ref, wv_ref, kc_ref, vc_ref, wp_ref, vl_ref,
             s_ref, f_ref, q_ref, end_ref, at_ref, kn_ref, vn_ref, k_ref, v_ref,
             hid, wqb, wkb, wvb, acc, mine, got, full, wp, vl,
             hsem, qsem, wsem, ksem, vsem, psem, s1, r1, s2, r2):
    me = lax.axis_index('sp')
    rows, seq, heads, dim = k_ref.shape
    depth, qw = wqb.shape
    blocks = dim // 128
    w = TILE * heads
    small = [
        pltpu.make_async_copy(hid_ref, hid, hsem),
        pltpu.make_async_copy(wp_ref, wp, psem.at[0]),
        pltpu.make_async_copy(vl_ref, vl, psem.at[1]),
    ]

    def slices(parts):
        unit = depth // sum(parts)
        return [pl.ds(sum(parts[:c]) * unit, parts[c] * unit) for c in range(len(parts))]

    q_rows, kv_rows = slices(Q_PARTS), slices(KV_PARTS)
    q_copies = [pltpu.make_async_copy(wq_ref.at[r, _rows(me, qw)], wqb.at[r], qsem.at[c]) for c, r in enumerate(q_rows)]
    kv_copies = [
        pltpu.make_async_copy(src.at[r, _rows(me, dim)], dst.at[r], wsem.at[i, c])
        for c, r in enumerate(kv_rows) for i, (src, dst) in enumerate(((wk_ref, wkb), (wv_ref, wvb)))
    ]
    k_copies, v_copies = [
        [pltpu.make_async_copy(src.at[_part(i, rows, parts)], dst.at[_part(i, rows, parts)], sem.at[i]) for i in range(parts)]
        for src, dst, sem, parts in ((kc_ref, k_ref, ksem, K_PARTS), (vc_ref, v_ref, vsem, V_PARTS))
    ]
    for cp in q_copies + small:
        cp.start()
    barrier = _greet(me, n)

    def gathered(i, ssem, rsem):
        return _exchange(me, n, lambda peer: mine.at[i], lambda off: got.at[i, off - 1], ssem, rsem)

    def spread(i, src, value):
        value = value.astype(F32)
        for c in range(value.shape[1] // 128):
            full[i * 2 * blocks + c, _rows(src, rows), :] = value[:, c * 128:(c + 1) * 128]

    def collect(i, copies):
        for off in range(1, n):
            copies[off - 1].wait()
            spread(i, _peer(me, n - off, n), got[i, off - 1])

    for cp in small:
        cp.wait()
    for c, r in enumerate(q_rows):
        q_copies[c].wait()
        if c == 0:
            for cp in kv_copies:
                cp.start()
        if c == len(q_rows) - 1:
            for cp in k_copies[:K_FIRST]:
                cp.start()

        @pl.when(me >= 0)
        def _():
            part = jnp.dot(hid[:, r], wqb[r, :], preferred_element_type=F32)
            acc[:, :qw] = part if c == 0 else acc[:, :qw] + part

    mine[0] = acc[:, :qw].astype(BF16)
    pl.semaphore_wait(barrier, n - 1)
    x1 = gathered(0, s1, r1)
    for c, r in enumerate(kv_rows):
        for cp in kv_copies[2 * c:2 * c + 2]:
            cp.wait()
        if c == 0:
            for cp in k_copies[K_FIRST:]:
                cp.start()

        @pl.when(me >= 0)
        def _():
            part = jnp.concatenate([jnp.dot(hid[:, r], ref[r, :], preferred_element_type=F32) for ref in (wkb, wvb)], axis=1)
            acc[:, qw:] = part if c == 0 else acc[:, qw:] + part

    mine[1] = acc[:, qw:].astype(BF16)
    x2 = gathered(1, s2, r2)
    for cp in v_copies:
        cp.start()
    for i in range(2):
        spread(i, me, mine[i])
    collect(0, x1)

    def of_row(b, first):
        return jnp.concatenate([full[first * blocks + c, pl.ds(b, n, stride=rows), :] for c in range(blocks)], axis=1)

    def times(q, kt):
        return lax.dot_general(q, kt, (((1,), (1,)), ((), ())), preferred_element_type=F32) * scale

    colpos = _positions(heads, w, 2 * seq * n)
    scale = dim ** -0.5
    for cp in k_copies:
        cp.wait()
    for b in range(rows):
        q = jnp.concatenate([of_row(b, 0), of_row(b, 1)], axis=0).astype(BF16)
        q_ref[b] = q
        end = vl[b] - me * seq
        end_ref[b:b + 1, :] = jnp.full((1, w), end, jnp.int32)
        if b >= EARLY:
            continue
        for t in range(seq // TILE):
            s = times(q, k_ref[b, pl.ds(t * TILE, TILE)].reshape(w, dim))
            s_ref[b, :, t * w:(t + 1) * w] = jnp.where(colpos < end - t * TILE, s, -jnp.inf)
    collect(1, x2)
    for b in range(rows):
        kn = of_row(b, 2).astype(BF16)
        kn_ref[b] = kn
        vn_ref[b] = of_row(b, 3).astype(BF16)
        at_ref[b:b + 1, :] = jnp.full((1, w), wp[b] - me * seq, jnp.int32)
        if b >= EARLY:
            continue
        s = times(q_ref[b], jnp.concatenate([kn[None]] * TILE, axis=0).reshape(w, dim))
        f_ref[b] = jnp.where(wp[b] < vl[b], s, -jnp.inf)
    for cp in v_copies:
        cp.wait()


def _patch(at_ref, kn_ref, vn_ref, ki_ref, vi_ref, k_ref, v_ref):
    del ki_ref, vi_ref
    rows, seq = k_ref.shape[:2]
    for b in range(rows):
        at = at_ref[b, 0]

        @pl.when((at >= 0) & (at < seq))
        def _():
            k_ref[b, at] = kn_ref[b]
            v_ref[b, at] = vn_ref[b]


def _attend(n, s_ref, f_ref, q_ref, end_ref, at_ref, k_ref, v_ref, wo_ref, out_ref, w_ref, p_ref, xs, xr, part, recv, red, gath,
            wsem, s2, r2, s4, r4, s5, r5):
    me = lax.axis_index('sp')
    rows, seq, heads, dim = v_ref.shape
    model = out_ref.shape[1]
    cols = red.shape[1]
    blocks = dim // 128
    ntile = seq // TILE
    w = TILE * heads
    span = xs.shape[0] // heads
    wcopy = pltpu.make_async_copy(wo_ref, w_ref.at[:, pl.ds(0, model)], wsem)
    wcopy.start()
    w_ref[:, model:] = jnp.zeros((w_ref.shape[0], n * cols - model), BF16)
    barrier = _greet(me, n)
    lane = lax.broadcasted_iota(jnp.int32, (heads, 128), 1)
    colpos = _positions(heads, w, 2 * seq * n)
    scale = dim ** -0.5

    def soften(b):
        if b < EARLY:
            at = at_ref[b:b + 1, :]
            fresh = f_ref[b]
            ss = [jnp.where(colpos == at - t * TILE, fresh, s_ref[b, :, t * w:(t + 1) * w]) for t in range(ntile)]
        else:
            end = end_ref[b:b + 1, :]
            ss = [lax.dot_general(q_ref[b], k_ref[b, pl.ds(t * TILE, TILE)].reshape(w, dim), (((1,), (1,)), ((), ())),
                                  preferred_element_type=F32) * scale for t in range(ntile)]
            ss = [jnp.where(colpos < end - t * TILE, s, -jnp.inf) for t, s in enumerate(ss)]
        m = jnp.max(functools.reduce(jnp.maximum, ss), axis=-1, keepdims=True)
        m = jnp.maximum(m, FLOOR)
        ps = [jnp.exp(s - m) for s in ss]
        l = jnp.sum(functools.reduce(jnp.add, ps), axis=-1, keepdims=True)
        for t in range(ntile):
            p_ref[b, :, t * w:(t + 1) * w] = ps[t].astype(BF16)
        st = jnp.where(lane == 0, m[:heads], jnp.where(lane == 1, l[:heads], jnp.where(lane == 2, m[heads:], l[heads:])))
        xs[pl.ds(blocks * 2 * rows + b, heads, stride=span), :] = st

    def values(b):
        acc = functools.reduce(jnp.add, [
            functools.reduce(jnp.add, [
                jnp.dot(p_ref[b, :, t * w:(t + 1) * w], v_ref[b, pl.ds(t * TILE, TILE)].reshape(w, dim),
                        preferred_element_type=F32) for t in range(first, ntile, 2)]) for first in range(2)])
        for c in range(blocks):
            piece = acc[:, c * 128:(c + 1) * 128]
            xs[pl.ds(c * 2 * rows + b, heads, stride=span), :] = piece[:heads]
            xs[pl.ds(c * 2 * rows + rows + b, heads, stride=span), :] = piece[heads:]

    for i in range(rows + LAG):
        if i < rows:
            soften(i)
        if i >= LAG:
            values(i - LAG)
    pl.semaphore_wait(barrier, n - 1)
    x2 = _exchange(me, n, lambda peer: xs.at[_rows(peer, span)], lambda off: xr.at[off - 1], s2, r2)
    xr[n - 1] = xs[_rows(me, span), :]
    for cp in x2:
        cp.wait()
    base = blocks * 2 * rows
    pieces = []
    sts = [xr[i, base:base + rows, :] for i in range(n)]
    for j in range(2):
        ms = [st[:, 2 * j:2 * j + 1] for st in sts]
        top = functools.reduce(jnp.maximum, ms)
        es = [jnp.exp(m - top) for m in ms]
        total = functools.reduce(jnp.add, [st[:, 2 * j + 1:2 * j + 2] * e for st, e in zip(sts, es)])
        for c in range(blocks):
            at = c * 2 * rows + j * rows
            num = functools.reduce(jnp.add, [xr[i, at:at + rows, :] * es[i] for i in range(n)])
            pieces.append((num / total).astype(BF16))
    o = jnp.concatenate(pieces, axis=1)
    wcopy.wait()

    def block(i):
        return jnp.dot(o, w_ref[:, _rows(i, cols)], preferred_element_type=F32)

    rs = []
    for off in _far_first(n):
        peer = _peer(me, off, n)
        part[off - 1] = block(peer)
        rs.append(pltpu.make_async_remote_copy(
            src_ref=part.at[off - 1], dst_ref=recv.at[off - 1], send_sem=s4.at[off - 1], recv_sem=r4.at[off - 1],
            device_id={'sp': peer}, device_id_type=MESH))
        rs[-1].start()
    total = block(me)
    for off in range(1, n):
        rs[_far_first(n).index(off)].wait()
        total += recv[off - 1]
    red[...] = total.astype(BF16)
    ag = _exchange(me, n, lambda peer: red, lambda off: gath.at[:, _rows(me, cols)], s5, r5)
    for cp in ag:
        cp.wait()
    gath[:, _rows(me, cols)] = red[...]
    out_ref[...] = gath[:, :model]


def _hand_over(attn_ref, k_ref, v_ref, out_ref):
    del k_ref, v_ref
    out_ref[...] = attn_ref[...]


def solution(mesh):
    row_spec = P(('rep', 'dp'), None)
    cache_spec = P(('rep', 'dp'), 'sp', None, None)
    len_spec = P(('rep', 'dp'))
    n = mesh.shape['sp']
    vmem = pl.BlockSpec(memory_space=pltpu.VMEM)
    hbm = pl.BlockSpec(memory_space=pltpu.HBM)
    dma = pltpu.SemaphoreType.DMA

    def in_hbm(x):
        return pltpu.with_memory_space_constraint(x, pltpu.HBM)

    def local_step(hidden, w_query, w_key, w_value, w_out, k_cache, v_cache, write_pos, valid_len):
        rows, seq, heads, dim = k_cache.shape
        depth = hidden.shape[1]
        model = w_out.shape[1]
        qw = w_query.shape[1] // n
        lw = qw + 2 * dim
        blocks = dim // 128
        cache = pltpu.VMEM(k_cache.shape, BF16)
        new = pltpu.VMEM((rows, heads, dim), BF16)
        scores, fresh, query, ends, at, k_new, v_new, k_here, v_here = pl.pallas_call(
            functools.partial(_project, n),
            out_shape=(
                pltpu.VMEM((EARLY, 2 * heads, seq * heads), F32),
                pltpu.VMEM((EARLY, 2 * heads, TILE * heads), F32),
                pltpu.VMEM((rows, 2 * heads, dim), BF16),
                pltpu.VMEM((rows, TILE * heads), jnp.int32),
                pltpu.VMEM((rows, TILE * heads), jnp.int32),
                new, new, cache, cache,
            ),
            in_specs=[hbm] * 8,
            out_specs=(vmem,) * 9,
            scratch_shapes=[
                pltpu.VMEM((rows, depth), BF16),
                pltpu.VMEM((depth, qw), BF16),
                pltpu.VMEM((depth, dim), BF16),
                pltpu.VMEM((depth, dim), BF16),
                pltpu.VMEM((rows, lw), F32),
                pltpu.VMEM((2, rows, lw // 2), BF16),
                pltpu.VMEM((2, n - 1, rows, lw // 2), BF16),
                pltpu.VMEM((lw // 128, n * rows, 128), F32),
                pltpu.SMEM((rows,), jnp.int32),
                pltpu.SMEM((rows,), jnp.int32),
                dma, dma((len(Q_PARTS),)), dma((2, len(KV_PARTS))), dma((K_PARTS,)), dma((V_PARTS,)), dma((2,)),
            ] + [dma((n - 1,))] * 4,
            compiler_params=pltpu.CompilerParams(collective_id=0, has_side_effects=True, vmem_limit_bytes=12 * MIB),
            cost_estimate=pl.CostEstimate(flops=10_000_000_000, bytes_accessed=28 * MIB, transcendentals=0),
            name='project',
        )(*[in_hbm(x) for x in (hidden, w_query, w_key, w_value, k_cache, v_cache, write_pos, valid_len)])
        k_here, v_here = pl.pallas_call(
            _patch,
            out_shape=(cache, cache),
            in_specs=[vmem] * 5,
            out_specs=(vmem, vmem),
            input_output_aliases={3: 0, 4: 1},
            compiler_params=pltpu.CompilerParams(vmem_limit_bytes=1 * MIB),
            name='patch',
        )(at, k_new, v_new, k_here, v_here)
        top = lax.optimization_barrier(jnp.full((), jnp.inf, BF16))
        k_next = jnp.minimum(k_here, top)
        v_next = jnp.minimum(v_here, top)
        padded = -(-model // (128 * n)) * 128 * n
        span = 2 * rows * blocks + rows
        attn = pl.pallas_call(
            functools.partial(_attend, n),
            out_shape=jax.ShapeDtypeStruct((rows, model), BF16),
            in_specs=[vmem] * 7 + [hbm],
            out_specs=vmem,
            scratch_shapes=[
                pltpu.VMEM((w_out.shape[0], padded), BF16),
                pltpu.VMEM((rows, 2 * heads, seq * heads), BF16),
                pltpu.VMEM((heads * span, 128), F32),
                pltpu.VMEM((n, span, 128), F32),
                pltpu.VMEM((n - 1, rows, padded // n), F32),
                pltpu.VMEM((n - 1, rows, padded // n), F32),
                pltpu.VMEM((rows, padded // n), BF16),
                pltpu.VMEM((rows, padded), BF16),
                dma,
            ] + [dma((n - 1,))] * 6,
            compiler_params=pltpu.CompilerParams(collective_id=1, has_side_effects=True, vmem_limit_bytes=8 * MIB),
            cost_estimate=pl.CostEstimate(flops=20_000_000_000, bytes_accessed=4 * MIB, transcendentals=0),
            name='attend',
        )(scores, fresh, query, ends, at, k_next, v_next, in_hbm(w_out))
        attn = pl.pallas_call(
            _hand_over,
            out_shape=jax.ShapeDtypeStruct((rows, model), BF16),
            in_specs=[vmem] * 3,
            out_specs=vmem,
            compiler_params=pltpu.CompilerParams(vmem_limit_bytes=1 * MIB),
            name='hand_over',
        )(attn, k_next, v_next)
        return attn, k_next, v_next

    return jax.shard_map(
        local_step, mesh=mesh,
        in_specs=(row_spec, P(), P(), P(), P('sp', None), cache_spec, cache_spec, len_spec, len_spec),
        out_specs=(row_spec, cache_spec, cache_spec), check_vma=False)
```

```python
import functools

import jax
import jax.numpy as jnp
from jax import lax
from jax.experimental import pallas as pl
from jax.experimental.pallas import tpu as pltpu
from jax.sharding import PartitionSpec as P

F32 = jnp.float32
BF16 = jnp.bfloat16
FLOOR = float(jnp.finfo(jnp.float32).min)
MESH = pl.DeviceIdType.MESH
Q_PARTS = (6, 5, 3)
KV_PARTS = (8, 6)
K_PARTS = 4
K_FIRST = 2
V_PARTS = 2
EARLY = 7
FAR = 2
TILE = 32
LAG = 2
MIB = 1 << 20


def _peer(me, off, n):
    return lax.rem(me + off, n)


def _greet(me, n):
    barrier = pltpu.get_barrier_semaphore()
    for off in range(1, n):
        pl.semaphore_signal(barrier, inc=1, device_id={'sp': _peer(me, off, n)}, device_id_type=MESH)
    return barrier


def _far_first(n):
    return sorted(range(1, n), key=lambda off: abs(off - n // 2))


def _send(me, n, off, src, dst, sems):
    peer = _peer(me, off, n)
    pltpu.make_async_remote_copy(
        src_ref=src(peer), dst_ref=dst(off), send_sem=sems.at[0], recv_sem=sems.at[1],
        device_id={'sp': peer}, device_id_type=MESH).start()


def _exchange(me, n, src, dst, sems):
    for off in _far_first(n):
        _send(me, n, off, src, dst, sems)


def _settle(total, sems):
    for i in range(2):
        pltpu.make_async_copy(total, total, sems.at[i]).wait()


def _part(i, size, parts):
    return pl.ds(i * size // parts, size // parts)


def _positions(heads, width, never):
    col = lax.broadcasted_iota(jnp.int32, (2 * heads, width), 1)
    row = lax.broadcasted_iota(jnp.int32, (2 * heads, width), 0)
    return jnp.where((col % heads) == (row % heads), col // heads, never)


def _rows(i, count):
    return pl.ds(pl.multiple_of(i * count, count), count)


def _project(n, hid_ref, wq_ref, wk_ref, wv_ref, kc_ref, vc_ref, wp_ref, vl_ref,
             s_ref, f_ref, q_ref, end_ref, at_ref, kn_ref, vn_ref, k_ref, v_ref,
             hid, wqb, wkb, wvb, acc, mine, got, full, wp, vl,
             hsem, qsem, wsem, ksem, vsem, psem, x1, x2):
    me = lax.axis_index('sp')
    rows, seq, heads, dim = k_ref.shape
    depth, qw = wqb.shape
    blocks = dim // 128
    w = TILE * heads
    small = [
        pltpu.make_async_copy(hid_ref, hid, hsem),
        pltpu.make_async_copy(wp_ref, wp, psem.at[0]),
        pltpu.make_async_copy(vl_ref, vl, psem.at[1]),
    ]

    def slices(parts):
        unit = depth // sum(parts)
        return [pl.ds(sum(parts[:c]) * unit, parts[c] * unit) for c in range(len(parts))]

    q_rows, kv_rows = slices(Q_PARTS), slices(KV_PARTS)
    q_copies = [pltpu.make_async_copy(wq_ref.at[r, _rows(me, qw)], wqb.at[r], qsem.at[c]) for c, r in enumerate(q_rows)]
    kv_copies = [
        pltpu.make_async_copy(src.at[r, _rows(me, dim)], dst.at[r], wsem.at[i, c])
        for c, r in enumerate(kv_rows) for i, (src, dst) in enumerate(((wk_ref, wkb), (wv_ref, wvb)))
    ]
    k_copies, v_copies = [
        [pltpu.make_async_copy(src.at[_part(i, rows, parts)], dst.at[_part(i, rows, parts)], sem.at[i]) for i in range(parts)]
        for src, dst, sem, parts in ((kc_ref, k_ref, ksem, K_PARTS), (vc_ref, v_ref, vsem, V_PARTS))
    ]
    for cp in q_copies + small:
        cp.start()
    barrier = _greet(me, n)

    def gather(i, sems):
        _exchange(me, n, lambda peer: mine.at[i], lambda off: got.at[i, off - 1], sems)

    def spread(i, src, value):
        value = value.astype(F32)
        for c in range(value.shape[1] // 128):
            full[i * 2 * blocks + c, _rows(src, rows), :] = value[:, c * 128:(c + 1) * 128]

    def collect(i, sems):
        _settle(got.at[i], sems)
        for off in range(1, n):
            spread(i, _peer(me, n - off, n), got[i, off - 1])

    for cp in small:
        cp.wait()
    for c, r in enumerate(q_rows):
        q_copies[c].wait()
        if c == 0:
            for cp in kv_copies:
                cp.start()
        if c == len(q_rows) - 1:
            for cp in k_copies[:K_FIRST]:
                cp.start()

        @pl.when(me >= 0)
        def _():
            part = jnp.dot(hid[:, r], wqb[r, :], preferred_element_type=F32)
            acc[:, :qw] = part if c == 0 else acc[:, :qw] + part

    mine[0] = acc[:, :qw].astype(BF16)
    pl.semaphore_wait(barrier, n - 1)
    gather(0, x1)
    for c, r in enumerate(kv_rows):
        for cp in kv_copies[2 * c:2 * c + 2]:
            cp.wait()
        if c == 0:
            for cp in k_copies[K_FIRST:]:
                cp.start()

        @pl.when(me >= 0)
        def _():
            part = jnp.concatenate([jnp.dot(hid[:, r], ref[r, :], preferred_element_type=F32) for ref in (wkb, wvb)], axis=1)
            acc[:, qw:] = part if c == 0 else acc[:, qw:] + part

    mine[1] = acc[:, qw:].astype(BF16)
    gather(1, x2)
    for cp in v_copies:
        cp.start()
    for i in range(2):
        spread(i, me, mine[i])
    collect(0, x1)

    def of_row(b, first):
        return jnp.concatenate([full[first * blocks + c, pl.ds(b, n, stride=rows), :] for c in range(blocks)], axis=1)

    def times(q, kt):
        return lax.dot_general(q, kt, (((1,), (1,)), ((), ())), preferred_element_type=F32) * scale

    colpos = _positions(heads, w, 2 * seq * n)
    scale = dim ** -0.5
    for cp in k_copies:
        cp.wait()
    for b in range(rows):
        q = jnp.concatenate([of_row(b, 0), of_row(b, 1)], axis=0).astype(BF16)
        q_ref[b] = q
        end = vl[b] - me * seq
        end_ref[b:b + 1, :] = jnp.full((1, w), end, jnp.int32)
        if b >= EARLY:
            continue
        for t in range(seq // TILE):
            s = times(q, k_ref[b, pl.ds(t * TILE, TILE)].reshape(w, dim))
            s_ref[b, :, t * w:(t + 1) * w] = jnp.where(colpos < end - t * TILE, s, -jnp.inf)
    collect(1, x2)
    for b in range(rows):
        kn = of_row(b, 2).astype(BF16)
        kn_ref[b] = kn
        vn_ref[b] = of_row(b, 3).astype(BF16)
        at_ref[b:b + 1, :] = jnp.full((1, w), wp[b] - me * seq, jnp.int32)
        if b >= EARLY:
            continue
        s = times(q_ref[b], jnp.concatenate([kn[None]] * TILE, axis=0).reshape(w, dim))
        f_ref[b] = jnp.where(wp[b] < vl[b], s, -jnp.inf)
    for cp in v_copies:
        cp.wait()


def _patch(at_ref, kn_ref, vn_ref, ki_ref, vi_ref, k_ref, v_ref):
    del ki_ref, vi_ref
    rows, seq = k_ref.shape[:2]
    for b in range(rows):
        at = at_ref[b, 0]

        @pl.when((at >= 0) & (at < seq))
        def _():
            k_ref[b, at] = kn_ref[b]
            v_ref[b, at] = vn_ref[b]


def _attend(n, s_ref, f_ref, q_ref, end_ref, at_ref, k_ref, v_ref, wo_ref, out_ref, w_ref, p_ref, xs, xr, part, recv, red, gath,
            wsem, x2, x3, x4):
    me = lax.axis_index('sp')
    rows, seq, heads, dim = v_ref.shape
    model = out_ref.shape[1]
    cols = red.shape[1]
    blocks = dim // 128
    ntile = seq // TILE
    w = TILE * heads
    span = xs.shape[0] // heads
    wcopy = pltpu.make_async_copy(wo_ref, w_ref.at[:, pl.ds(0, model)], wsem)
    wcopy.start()
    w_ref[:, model:] = jnp.zeros((w_ref.shape[0], n * cols - model), BF16)
    barrier = _greet(me, n)
    lane = lax.broadcasted_iota(jnp.int32, (heads, 128), 1)
    colpos = _positions(heads, w, 2 * seq * n)
    scale = dim ** -0.5

    def soften(b):
        if b < EARLY:
            at = at_ref[b:b + 1, :]
            fresh = f_ref[b]
            ss = [jnp.where(colpos == at - t * TILE, fresh, s_ref[b, :, t * w:(t + 1) * w]) for t in range(ntile)]
        else:
            end = end_ref[b:b + 1, :]
            ss = [lax.dot_general(q_ref[b], k_ref[b, pl.ds(t * TILE, TILE)].reshape(w, dim), (((1,), (1,)), ((), ())),
                                  preferred_element_type=F32) * scale for t in range(ntile)]
            ss = [jnp.where(colpos < end - t * TILE, s, -jnp.inf) for t, s in enumerate(ss)]
        m = jnp.max(functools.reduce(jnp.maximum, ss), axis=-1, keepdims=True)
        m = jnp.maximum(m, FLOOR)
        ps = [jnp.exp(s - m) for s in ss]
        l = jnp.sum(functools.reduce(jnp.add, ps), axis=-1, keepdims=True)
        for t in range(ntile):
            p_ref[b, :, t * w:(t + 1) * w] = ps[t].astype(BF16)
        st = jnp.where(lane == 0, m[:heads], jnp.where(lane == 1, l[:heads], jnp.where(lane == 2, m[heads:], l[heads:])))
        xs[pl.ds(blocks * 2 * rows + b, heads, stride=span), :] = st

    def values(b):
        acc = functools.reduce(jnp.add, [
            functools.reduce(jnp.add, [
                jnp.dot(p_ref[b, :, t * w:(t + 1) * w], v_ref[b, pl.ds(t * TILE, TILE)].reshape(w, dim),
                        preferred_element_type=F32) for t in range(first, ntile, 2)]) for first in range(2)])
        for c in range(blocks):
            piece = acc[:, c * 128:(c + 1) * 128]
            xs[pl.ds(c * 2 * rows + b, heads, stride=span), :] = piece[:heads]
            xs[pl.ds(c * 2 * rows + rows + b, heads, stride=span), :] = piece[heads:]

    for i in range(rows + LAG):
        if i < rows:
            soften(i)
        if i >= LAG:
            values(i - LAG)
    pl.semaphore_wait(barrier, n - 1)
    _exchange(me, n, lambda peer: xs.at[_rows(peer, span)], lambda off: xr.at[off - 1], x2)
    xr[n - 1] = xs[_rows(me, span), :]
    _settle(xr.at[pl.ds(0, n - 1)], x2)
    base = blocks * 2 * rows
    pieces = []
    sts = [xr[i, base:base + rows, :] for i in range(n)]
    for j in range(2):
        ms = [st[:, 2 * j:2 * j + 1] for st in sts]
        top = functools.reduce(jnp.maximum, ms)
        es = [jnp.exp(m - top) for m in ms]
        total = functools.reduce(jnp.add, [st[:, 2 * j + 1:2 * j + 2] * e for st, e in zip(sts, es)])
        for c in range(blocks):
            at = c * 2 * rows + j * rows
            num = functools.reduce(jnp.add, [xr[i, at:at + rows, :] * es[i] for i in range(n)])
            pieces.append((num / total).astype(BF16))
    o = jnp.concatenate(pieces, axis=1)
    wcopy.wait()

    order = _far_first(n)
    for group in (order[:FAR], order[FAR:]):
        for off in group:
            part[off - 1] = jnp.dot(o, w_ref[:, _rows(_peer(me, off, n), cols)], preferred_element_type=F32)
        for off in group:
            _send(me, n, off, lambda peer: part.at[off - 1], lambda off: recv.at[off - 1], x3)
    total = jnp.dot(o, w_ref[:, _rows(me, cols)], preferred_element_type=F32)
    _settle(recv, x3)
    for off in range(1, n):
        total += recv[off - 1]
    red[...] = total.astype(BF16)
    _exchange(me, n, lambda peer: red, lambda off: gath.at[:, _rows(me, cols)], x4)
    _settle(gath.at[:, pl.ds(0, (n - 1) * cols)], x4)
    gath[:, _rows(me, cols)] = red[...]
    out_ref[...] = gath[:, :model]


def _hand_over(attn_ref, k_ref, v_ref, out_ref):
    del k_ref, v_ref
    out_ref[...] = attn_ref[...]


def solution(mesh):
    row_spec = P(('rep', 'dp'), None)
    cache_spec = P(('rep', 'dp'), 'sp', None, None)
    len_spec = P(('rep', 'dp'))
    n = mesh.shape['sp']
    vmem = pl.BlockSpec(memory_space=pltpu.VMEM)
    hbm = pl.BlockSpec(memory_space=pltpu.HBM)
    dma = pltpu.SemaphoreType.DMA

    def in_hbm(x):
        return pltpu.with_memory_space_constraint(x, pltpu.HBM)

    def local_step(hidden, w_query, w_key, w_value, w_out, k_cache, v_cache, write_pos, valid_len):
        rows, seq, heads, dim = k_cache.shape
        depth = hidden.shape[1]
        model = w_out.shape[1]
        qw = w_query.shape[1] // n
        lw = qw + 2 * dim
        blocks = dim // 128
        cache = pltpu.VMEM(k_cache.shape, BF16)
        new = pltpu.VMEM((rows, heads, dim), BF16)
        scores, fresh, query, ends, at, k_new, v_new, k_here, v_here = pl.pallas_call(
            functools.partial(_project, n),
            out_shape=(
                pltpu.VMEM((EARLY, 2 * heads, seq * heads), F32),
                pltpu.VMEM((EARLY, 2 * heads, TILE * heads), F32),
                pltpu.VMEM((rows, 2 * heads, dim), BF16),
                pltpu.VMEM((rows, TILE * heads), jnp.int32),
                pltpu.VMEM((rows, TILE * heads), jnp.int32),
                new, new, cache, cache,
            ),
            in_specs=[hbm] * 8,
            out_specs=(vmem,) * 9,
            scratch_shapes=[
                pltpu.VMEM((rows, depth), BF16),
                pltpu.VMEM((depth, qw), BF16),
                pltpu.VMEM((depth, dim), BF16),
                pltpu.VMEM((depth, dim), BF16),
                pltpu.VMEM((rows, lw), F32),
                pltpu.VMEM((2, rows, lw // 2), BF16),
                pltpu.VMEM((2, n - 1, rows, lw // 2), BF16),
                pltpu.VMEM((lw // 128, n * rows, 128), F32),
                pltpu.SMEM((rows,), jnp.int32),
                pltpu.SMEM((rows,), jnp.int32),
                dma, dma((len(Q_PARTS),)), dma((2, len(KV_PARTS))), dma((K_PARTS,)), dma((V_PARTS,)), dma((2,)),
                dma((2,)), dma((2,)),
            ],
            compiler_params=pltpu.CompilerParams(collective_id=0, has_side_effects=True, vmem_limit_bytes=12 * MIB),
            cost_estimate=pl.CostEstimate(flops=10_000_000_000, bytes_accessed=28 * MIB, transcendentals=0),
            name='project',
        )(*[in_hbm(x) for x in (hidden, w_query, w_key, w_value, k_cache, v_cache, write_pos, valid_len)])
        k_here, v_here = pl.pallas_call(
            _patch,
            out_shape=(cache, cache),
            in_specs=[vmem] * 5,
            out_specs=(vmem, vmem),
            input_output_aliases={3: 0, 4: 1},
            compiler_params=pltpu.CompilerParams(vmem_limit_bytes=1 * MIB),
            name='patch',
        )(at, k_new, v_new, k_here, v_here)
        top = lax.optimization_barrier(jnp.full((), jnp.inf, BF16))
        k_next = jnp.minimum(k_here, top)
        v_next = jnp.minimum(v_here, top)
        padded = -(-model // (128 * n)) * 128 * n
        span = 2 * rows * blocks + rows
        attn = pl.pallas_call(
            functools.partial(_attend, n),
            out_shape=jax.ShapeDtypeStruct((rows, model), BF16),
            in_specs=[vmem] * 7 + [hbm],
            out_specs=vmem,
            scratch_shapes=[
                pltpu.VMEM((w_out.shape[0], padded), BF16),
                pltpu.VMEM((rows, 2 * heads, seq * heads), BF16),
                pltpu.VMEM((heads * span, 128), F32),
                pltpu.VMEM((n, span, 128), F32),
                pltpu.VMEM((n - 1, rows, padded // n), F32),
                pltpu.VMEM((n - 1, rows, padded // n), F32),
                pltpu.VMEM((rows, padded // n), BF16),
                pltpu.VMEM((rows, padded), BF16),
                dma, dma((2,)), dma((2,)), dma((2,)),
            ],
            compiler_params=pltpu.CompilerParams(collective_id=1, has_side_effects=True, vmem_limit_bytes=8 * MIB),
            cost_estimate=pl.CostEstimate(flops=20_000_000_000, bytes_accessed=4 * MIB, transcendentals=0),
            name='attend',
        )(scores, fresh, query, ends, at, k_next, v_next, in_hbm(w_out))
        attn = pl.pallas_call(
            _hand_over,
            out_shape=jax.ShapeDtypeStruct((rows, model), BF16),
            in_specs=[vmem] * 3,
            out_specs=vmem,
            compiler_params=pltpu.CompilerParams(vmem_limit_bytes=1 * MIB),
            name='hand_over',
        )(attn, k_next, v_next)
        return attn, k_next, v_next

    return jax.shard_map(
        local_step, mesh=mesh,
        in_specs=(row_spec, P(), P(), P(), P('sp', None), cache_spec, cache_spec, len_spec, len_spec),
        out_specs=(row_spec, cache_spec, cache_spec), check_vma=False)
```

```python
import functools

import jax
import jax.numpy as jnp
from jax import lax
from jax.experimental import pallas as pl
from jax.experimental.pallas import tpu as pltpu
from jax.sharding import PartitionSpec as P

F32 = jnp.float32
BF16 = jnp.bfloat16
FLOOR = float(jnp.finfo(jnp.float32).min)
MESH = pl.DeviceIdType.MESH
Q_PARTS = (6, 5, 3)
KV_PARTS = (8, 6)
K_PARTS = 2
K_FIRST = 1
V_PARTS = 1
EARLY = 7
GROUPS = ((0,), (1, 2), (3, 4), (5, 6))
TILE = 32
LAG = 3
MIB = 1 << 20


def _peer(me, off, n):
    return lax.rem(me + off, n)


def _greet(me, n):
    barrier = pltpu.get_barrier_semaphore()
    for off in range(1, n):
        pl.semaphore_signal(barrier, inc=1, device_id={'sp': _peer(me, off, n)}, device_id_type=MESH)
    return barrier


def _far_first(n):
    return sorted(range(1, n), key=lambda off: abs(off - n // 2))


def _send(me, n, off, src, dst, sems):
    peer = _peer(me, off, n)
    pltpu.make_async_remote_copy(
        src_ref=src(peer), dst_ref=dst(off), send_sem=sems.at[0], recv_sem=sems.at[1],
        device_id={'sp': peer}, device_id_type=MESH).start()


def _exchange(me, n, src, dst, sems):
    for off in _far_first(n):
        _send(me, n, off, src, dst, sems)


def _settle(total, sems):
    for i in range(2):
        pltpu.make_async_copy(total, total, sems.at[i]).wait()


def _part(i, size, parts):
    return pl.ds(i * size // parts, size // parts)


def _positions(heads, width, never):
    col = lax.broadcasted_iota(jnp.int32, (2 * heads, width), 1)
    row = lax.broadcasted_iota(jnp.int32, (2 * heads, width), 0)
    return jnp.where((col % heads) == (row % heads), col // heads, never)


def _rows(i, count):
    return pl.ds(pl.multiple_of(i * count, count), count)


def _project(n, hid_ref, wq_ref, wk_ref, wv_ref, kc_ref, vc_ref, wp_ref, vl_ref,
             s_ref, f_ref, q_ref, end_ref, at_ref, kn_ref, vn_ref, k_ref, v_ref,
             hid, wqb, wkb, wvb, acc, mine, got, full, wp, vl,
             hsem, qsem, wsem, ksem, vsem, psem, x1, x2):
    me = lax.axis_index('sp')
    rows, seq, heads, dim = k_ref.shape
    depth, qw = wqb.shape
    blocks = dim // 128
    w = TILE * heads
    small = [
        pltpu.make_async_copy(hid_ref, hid, hsem),
        pltpu.make_async_copy(wp_ref, wp, psem.at[0]),
        pltpu.make_async_copy(vl_ref, vl, psem.at[1]),
    ]

    def slices(parts):
        unit = depth // sum(parts)
        return [pl.ds(sum(parts[:c]) * unit, parts[c] * unit) for c in range(len(parts))]

    q_rows, kv_rows = slices(Q_PARTS), slices(KV_PARTS)
    q_copies = [pltpu.make_async_copy(wq_ref.at[r, _rows(me, qw)], wqb.at[r], qsem.at[c]) for c, r in enumerate(q_rows)]
    kv_copies = [
        pltpu.make_async_copy(src.at[r, _rows(me, dim)], dst.at[r], wsem.at[i, c])
        for c, r in enumerate(kv_rows) for i, (src, dst) in enumerate(((wk_ref, wkb), (wv_ref, wvb)))
    ]
    k_copies, v_copies = [
        [pltpu.make_async_copy(src.at[_part(i, rows, parts)], dst.at[_part(i, rows, parts)], sem.at[i]) for i in range(parts)]
        for src, dst, sem, parts in ((kc_ref, k_ref, ksem, K_PARTS), (vc_ref, v_ref, vsem, V_PARTS))
    ]
    for cp in q_copies + small:
        cp.start()
    barrier = _greet(me, n)

    def gather(i, sems):
        _exchange(me, n, lambda peer: mine.at[i], lambda off: got.at[i, off - 1], sems)

    def spread(i, src, value):
        value = value.astype(F32)
        for c in range(value.shape[1] // 128):
            full[i * 2 * blocks + c, _rows(src, rows), :] = value[:, c * 128:(c + 1) * 128]

    def collect(i, sems):
        _settle(got.at[i], sems)
        for off in range(1, n):
            spread(i, _peer(me, n - off, n), got[i, off - 1])

    for cp in small:
        cp.wait()
    for c, r in enumerate(q_rows):
        q_copies[c].wait()
        if c == 0:
            for cp in kv_copies:
                cp.start()
        if c == len(q_rows) - 1:
            for cp in k_copies[:K_FIRST]:
                cp.start()

        @pl.when(me >= 0)
        def _():
            part = jnp.dot(hid[:, r], wqb[r, :], preferred_element_type=F32)
            acc[:, :qw] = part if c == 0 else acc[:, :qw] + part

    mine[0] = acc[:, :qw].astype(BF16)
    pl.semaphore_wait(barrier, n - 1)
    gather(0, x1)
    for c, r in enumerate(kv_rows):
        for cp in kv_copies[2 * c:2 * c + 2]:
            cp.wait()
        if c == 0:
            for cp in k_copies[K_FIRST:]:
                cp.start()

        @pl.when(me >= 0)
        def _():
            part = jnp.concatenate([jnp.dot(hid[:, r], ref[r, :], preferred_element_type=F32) for ref in (wkb, wvb)], axis=1)
            acc[:, qw:] = part if c == 0 else acc[:, qw:] + part

    mine[1] = acc[:, qw:].astype(BF16)
    gather(1, x2)
    for cp in v_copies:
        cp.start()
    for i in range(2):
        spread(i, me, mine[i])
    collect(0, x1)

    def of_row(b, first):
        return jnp.concatenate([full[first * blocks + c, pl.ds(b, n, stride=rows), :] for c in range(blocks)], axis=1)

    def times(q, kt):
        return lax.dot_general(q, kt, (((1,), (1,)), ((), ())), preferred_element_type=F32) * scale

    colpos = _positions(heads, w, 2 * seq * n)
    scale = dim ** -0.5
    for cp in k_copies:
        cp.wait()
    for b in range(rows):
        q = jnp.concatenate([of_row(b, 0), of_row(b, 1)], axis=0).astype(BF16)
        q_ref[b] = q
        end = vl[b] - me * seq
        end_ref[b:b + 1, :] = jnp.full((1, w), end, jnp.int32)
        if b >= EARLY:
            continue
        for t in range(seq // TILE):
            s = times(q, k_ref[b, pl.ds(t * TILE, TILE)].reshape(w, dim))
            s_ref[b, :, t * w:(t + 1) * w] = jnp.where(colpos < end - t * TILE, s, -jnp.inf)
    collect(1, x2)
    for b in range(rows):
        kn = of_row(b, 2).astype(BF16)
        kn_ref[b] = kn
        vn_ref[b] = of_row(b, 3).astype(BF16)
        at_ref[b:b + 1, :] = jnp.full((1, w), wp[b] - me * seq, jnp.int32)
        if b >= EARLY:
            continue
        s = times(q_ref[b], jnp.concatenate([kn[None]] * TILE, axis=0).reshape(w, dim))
        f_ref[b] = jnp.where(wp[b] < vl[b], s, -jnp.inf)
    for cp in v_copies:
        cp.wait()


def _patch(at_ref, kn_ref, vn_ref, ki_ref, vi_ref, k_ref, v_ref):
    del ki_ref, vi_ref
    rows, seq = k_ref.shape[:2]
    ats = [at_ref[b, 0] for b in range(rows)]
    for b, at in enumerate(ats):
        @pl.when((at >= 0) & (at < seq))
        def _():
            k_ref[b, at] = kn_ref[b]
            v_ref[b, at] = vn_ref[b]


def _attend(n, s_ref, f_ref, q_ref, end_ref, at_ref, k_ref, v_ref, wo_ref, out_ref, w_ref, p_ref, xs, xr, part, recv, red, gath,
            wsem, x2, x3, x4):
    me = lax.axis_index('sp')
    rows, seq, heads, dim = v_ref.shape
    model = out_ref.shape[1]
    cols = red.shape[1]
    blocks = dim // 128
    ntile = seq // TILE
    w = TILE * heads
    span = xs.shape[0] // heads
    wcopy = pltpu.make_async_copy(wo_ref, w_ref.at[:, pl.ds(0, model)], wsem)
    wcopy.start()
    w_ref[:, model:] = jnp.zeros((w_ref.shape[0], n * cols - model), BF16)
    barrier = _greet(me, n)
    lane = lax.broadcasted_iota(jnp.int32, (heads, 128), 1)
    colpos = _positions(heads, w, 2 * seq * n)
    scale = dim ** -0.5

    def soften(b):
        if b < EARLY:
            at = at_ref[b:b + 1, :]
            fresh = f_ref[b]
            ss = [jnp.where(colpos == at - t * TILE, fresh, s_ref[b, :, t * w:(t + 1) * w]) for t in range(ntile)]
        else:
            end = end_ref[b:b + 1, :]
            ss = [lax.dot_general(q_ref[b], k_ref[b, pl.ds(t * TILE, TILE)].reshape(w, dim), (((1,), (1,)), ((), ())),
                                  preferred_element_type=F32) * scale for t in range(ntile)]
            ss = [jnp.where(colpos < end - t * TILE, s, -jnp.inf) for t, s in enumerate(ss)]
        m = jnp.max(functools.reduce(jnp.maximum, ss), axis=-1, keepdims=True)
        m = jnp.maximum(m, FLOOR)
        ps = [jnp.exp(s - m) for s in ss]
        l = jnp.sum(functools.reduce(jnp.add, ps), axis=-1, keepdims=True)
        for t in range(ntile):
            p_ref[b, :, t * w:(t + 1) * w] = ps[t].astype(BF16)
        st = jnp.where(lane == 0, m[:heads], jnp.where(lane == 1, l[:heads], jnp.where(lane == 2, m[heads:], l[heads:])))
        xs[pl.ds(blocks * 2 * rows + b, heads, stride=span), :] = st

    def values(b):
        acc = functools.reduce(jnp.add, [
            functools.reduce(jnp.add, [
                jnp.dot(p_ref[b, :, t * w:(t + 1) * w], v_ref[b, pl.ds(t * TILE, TILE)].reshape(w, dim),
                        preferred_element_type=F32) for t in range(first, ntile, 2)]) for first in range(2)])
        for c in range(blocks):
            piece = acc[:, c * 128:(c + 1) * 128]
            xs[pl.ds(c * 2 * rows + b, heads, stride=span), :] = piece[:heads]
            xs[pl.ds(c * 2 * rows + rows + b, heads, stride=span), :] = piece[heads:]

    for i in range(rows + LAG):
        if i < rows:
            soften(i)
        if i >= LAG:
            values(i - LAG)
    pl.semaphore_wait(barrier, n - 1)
    _exchange(me, n, lambda peer: xs.at[_rows(peer, span)], lambda off: xr.at[off - 1], x2)
    xr[n - 1] = xs[_rows(me, span), :]
    _settle(xr.at[pl.ds(0, n - 1)], x2)
    base = blocks * 2 * rows
    pieces = []
    sts = [xr[i, base:base + rows, :] for i in range(n)]
    for j in range(2):
        ms = [st[:, 2 * j:2 * j + 1] for st in sts]
        top = functools.reduce(jnp.maximum, ms)
        es = [jnp.exp(m - top) for m in ms]
        total = functools.reduce(jnp.add, [st[:, 2 * j + 1:2 * j + 2] * e for st, e in zip(sts, es)])
        for c in range(blocks):
            at = c * 2 * rows + j * rows
            num = functools.reduce(jnp.add, [xr[i, at:at + rows, :] * es[i] for i in range(n)])
            pieces.append((num / total).astype(BF16))
    o = jnp.concatenate(pieces, axis=1)
    wcopy.wait()

    order = _far_first(n)
    for group in GROUPS:
        for i in group:
            off = order[i]
            part[off - 1] = jnp.dot(o, w_ref[:, _rows(_peer(me, off, n), cols)], preferred_element_type=F32)
        for i in group:
            off = order[i]
            _send(me, n, off, lambda peer: part.at[off - 1], lambda off: recv.at[off - 1], x3)
    part[n - 1] = jnp.dot(o, w_ref[:, _rows(me, cols)], preferred_element_type=F32)
    _settle(recv, x3)
    total = part[n - 1]
    for off in range(1, n):
        total += recv[off - 1]
    red[...] = total.astype(BF16)
    _exchange(me, n, lambda peer: red, lambda off: gath.at[:, _rows(me, cols)], x4)
    _settle(gath.at[:, pl.ds(0, (n - 1) * cols)], x4)
    gath[:, _rows(me, cols)] = red[...]
    out_ref[...] = gath[:, :model]


def _hand_over(attn_ref, k_ref, v_ref, out_ref):
    del k_ref, v_ref
    out_ref[...] = attn_ref[...]


def solution(mesh):
    row_spec = P(('rep', 'dp'), None)
    cache_spec = P(('rep', 'dp'), 'sp', None, None)
    len_spec = P(('rep', 'dp'))
    n = mesh.shape['sp']
    vmem = pl.BlockSpec(memory_space=pltpu.VMEM)
    hbm = pl.BlockSpec(memory_space=pltpu.HBM)
    dma = pltpu.SemaphoreType.DMA

    def in_hbm(x):
        return pltpu.with_memory_space_constraint(x, pltpu.HBM)

    def local_step(hidden, w_query, w_key, w_value, w_out, k_cache, v_cache, write_pos, valid_len):
        rows, seq, heads, dim = k_cache.shape
        depth = hidden.shape[1]
        model = w_out.shape[1]
        qw = w_query.shape[1] // n
        lw = qw + 2 * dim
        blocks = dim // 128
        cache = pltpu.VMEM(k_cache.shape, BF16)
        new = pltpu.VMEM((rows, heads, dim), BF16)
        scores, fresh, query, ends, at, k_new, v_new, k_here, v_here = pl.pallas_call(
            functools.partial(_project, n),
            out_shape=(
                pltpu.VMEM((EARLY, 2 * heads, seq * heads), F32),
                pltpu.VMEM((EARLY, 2 * heads, TILE * heads), F32),
                pltpu.VMEM((rows, 2 * heads, dim), BF16),
                pltpu.VMEM((rows, TILE * heads), jnp.int32),
                pltpu.VMEM((rows, TILE * heads), jnp.int32),
                new, new, cache, cache,
            ),
            in_specs=[hbm] * 8,
            out_specs=(vmem,) * 9,
            scratch_shapes=[
                pltpu.VMEM((rows, depth), BF16),
                pltpu.VMEM((depth, qw), BF16),
                pltpu.VMEM((depth, dim), BF16),
                pltpu.VMEM((depth, dim), BF16),
                pltpu.VMEM((rows, lw), F32),
                pltpu.VMEM((2, rows, lw // 2), BF16),
                pltpu.VMEM((2, n - 1, rows, lw // 2), BF16),
                pltpu.VMEM((lw // 128, n * rows, 128), F32),
                pltpu.SMEM((rows,), jnp.int32),
                pltpu.SMEM((rows,), jnp.int32),
                dma, dma((len(Q_PARTS),)), dma((2, len(KV_PARTS))), dma((K_PARTS,)), dma((V_PARTS,)), dma((2,)),
                dma((2,)), dma((2,)),
            ],
            compiler_params=pltpu.CompilerParams(collective_id=0, has_side_effects=True, vmem_limit_bytes=12 * MIB),
            cost_estimate=pl.CostEstimate(flops=10_000_000_000, bytes_accessed=28 * MIB, transcendentals=0),
            name='project',
        )(*[in_hbm(x) for x in (hidden, w_query, w_key, w_value, k_cache, v_cache, write_pos, valid_len)])
        k_here, v_here = pl.pallas_call(
            _patch,
            out_shape=(cache, cache),
            in_specs=[vmem] * 5,
            out_specs=(vmem, vmem),
            input_output_aliases={3: 0, 4: 1},
            compiler_params=pltpu.CompilerParams(vmem_limit_bytes=1 * MIB),
            name='patch',
        )(at, k_new, v_new, k_here, v_here)
        top = lax.optimization_barrier(jnp.full((), jnp.inf, BF16))
        k_next = jnp.minimum(k_here, top)
        v_next = jnp.minimum(v_here, top)
        padded = -(-model // (128 * n)) * 128 * n
        span = 2 * rows * blocks + rows
        attn = pl.pallas_call(
            functools.partial(_attend, n),
            out_shape=jax.ShapeDtypeStruct((rows, model), BF16),
            in_specs=[vmem] * 7 + [hbm],
            out_specs=vmem,
            scratch_shapes=[
                pltpu.VMEM((w_out.shape[0], padded), BF16),
                pltpu.VMEM((rows, 2 * heads, seq * heads), BF16),
                pltpu.VMEM((heads * span, 128), F32),
                pltpu.VMEM((n, span, 128), F32),
                pltpu.VMEM((n, rows, padded // n), F32),
                pltpu.VMEM((n - 1, rows, padded // n), F32),
                pltpu.VMEM((rows, padded // n), BF16),
                pltpu.VMEM((rows, padded), BF16),
                dma, dma((2,)), dma((2,)), dma((2,)),
            ],
            compiler_params=pltpu.CompilerParams(collective_id=1, has_side_effects=True, vmem_limit_bytes=8 * MIB),
            cost_estimate=pl.CostEstimate(flops=20_000_000_000, bytes_accessed=4 * MIB, transcendentals=0),
            name='attend',
        )(scores, fresh, query, ends, at, k_next, v_next, in_hbm(w_out))
        attn = pl.pallas_call(
            _hand_over,
            out_shape=jax.ShapeDtypeStruct((rows, model), BF16),
            in_specs=[vmem] * 3,
            out_specs=vmem,
            compiler_params=pltpu.CompilerParams(vmem_limit_bytes=1 * MIB),
            name='hand_over',
        )(attn, k_next, v_next)
        return attn, k_next, v_next

    return jax.shard_map(
        local_step, mesh=mesh,
        in_specs=(row_spec, P(), P(), P(), P('sp', None), cache_spec, cache_spec, len_spec, len_spec),
        out_specs=(row_spec, cache_spec, cache_spec), check_vma=False)
```

```python
import functools

import jax
import jax.numpy as jnp
from jax import lax
from jax.experimental import pallas as pl
from jax.experimental.pallas import tpu as pltpu
from jax.sharding import PartitionSpec as P

F32 = jnp.float32
BF16 = jnp.bfloat16
FLOOR = float(jnp.finfo(jnp.float32).min)
MESH = pl.DeviceIdType.MESH
Q_PARTS = (6, 5, 3)
KV_PARTS = (8, 6)
K_PARTS = 2
K_FIRST = 1
V_PARTS = 1
EARLY = 7
GROUPS = ((0,), (1, 2), (3, 4), (5, 6))
TILE = 32
LAG = 3
MIB = 1 << 20


def _peer(me, off, n):
    return lax.rem(me + off, n)


def _greet(me, n):
    barrier = pltpu.get_barrier_semaphore()
    for off in range(1, n):
        pl.semaphore_signal(barrier, inc=1, device_id={'sp': _peer(me, off, n)}, device_id_type=MESH)
    return barrier


def _far_first(n):
    return sorted(range(1, n), key=lambda off: abs(off - n // 2))


def _send(me, n, off, src, dst, sems):
    peer = _peer(me, off, n)
    pltpu.make_async_remote_copy(
        src_ref=src(peer), dst_ref=dst(off), send_sem=sems.at[0], recv_sem=sems.at[1],
        device_id={'sp': peer}, device_id_type=MESH).start()


def _exchange(me, n, src, dst, sems):
    for off in _far_first(n):
        _send(me, n, off, src, dst, sems)


def _settle(total, sems):
    for i in range(2):
        pltpu.make_async_copy(total, total, sems.at[i]).wait()


def _part(i, size, parts):
    return pl.ds(i * size // parts, size // parts)


def _positions(heads, width, never):
    col = lax.broadcasted_iota(jnp.int32, (2 * heads, width), 1)
    row = lax.broadcasted_iota(jnp.int32, (2 * heads, width), 0)
    return jnp.where((col % heads) == (row % heads), col // heads, never)


def _rows(i, count):
    return pl.ds(pl.multiple_of(i * count, count), count)


def _project(n, hid_ref, wq_ref, wk_ref, wv_ref, kc_ref, vc_ref, wp_ref, vl_ref,
             s_ref, f_ref, q_ref, end_ref, at_ref, kn_ref, vn_ref, k_ref, v_ref,
             hid, wqb, wkb, wvb, acc, mine, got, full, wp, vl,
             hsem, qsem, wsem, ksem, vsem, psem, x1, x2):
    me = lax.axis_index('sp')
    rows, seq, heads, dim = k_ref.shape
    depth, qw = wqb.shape
    blocks = dim // 128
    w = TILE * heads
    small = [
        pltpu.make_async_copy(hid_ref, hid, hsem),
        pltpu.make_async_copy(wp_ref, wp, psem.at[0]),
        pltpu.make_async_copy(vl_ref, vl, psem.at[1]),
    ]

    def slices(parts):
        unit = depth // sum(parts)
        return [pl.ds(sum(parts[:c]) * unit, parts[c] * unit) for c in range(len(parts))]

    q_rows, kv_rows = slices(Q_PARTS), slices(KV_PARTS)
    q_copies = [pltpu.make_async_copy(wq_ref.at[r, _rows(me, qw)], wqb.at[r], qsem.at[c]) for c, r in enumerate(q_rows)]
    kv_copies = [
        pltpu.make_async_copy(src.at[r, _rows(me, dim)], dst.at[r], wsem.at[i, c])
        for c, r in enumerate(kv_rows) for i, (src, dst) in enumerate(((wk_ref, wkb), (wv_ref, wvb)))
    ]
    k_copies, v_copies = [
        [pltpu.make_async_copy(src.at[_part(i, rows, parts)], dst.at[_part(i, rows, parts)], sem.at[i]) for i in range(parts)]
        for src, dst, sem, parts in ((kc_ref, k_ref, ksem, K_PARTS), (vc_ref, v_ref, vsem, V_PARTS))
    ]
    for cp in q_copies + small:
        cp.start()
    barrier = _greet(me, n)

    def gather(i, sems):
        _exchange(me, n, lambda peer: mine.at[i], lambda off: got.at[i, off - 1], sems)

    def spread(i, src, value):
        value = value.astype(F32)
        for c in range(value.shape[1] // 128):
            full[i * 2 * blocks + c, _rows(src, rows), :] = value[:, c * 128:(c + 1) * 128]

    def collect(i, sems):
        _settle(got.at[i], sems)
        for off in range(1, n):
            spread(i, _peer(me, n - off, n), got[i, off - 1])

    for cp in small:
        cp.wait()
    for c, r in enumerate(q_rows):
        q_copies[c].wait()
        if c == 0:
            for cp in kv_copies:
                cp.start()
        if c == len(q_rows) - 1:
            for cp in k_copies[:K_FIRST]:
                cp.start()

        @pl.when(me >= 0)
        def _():
            part = jnp.dot(hid[:, r], wqb[r, :], preferred_element_type=F32)
            acc[:, :qw] = part if c == 0 else acc[:, :qw] + part

    mine[0] = acc[:, :qw].astype(BF16)
    pl.semaphore_wait(barrier, n - 1)
    gather(0, x1)
    for c, r in enumerate(kv_rows):
        for cp in kv_copies[2 * c:2 * c + 2]:
            cp.wait()
        if c == 0:
            for cp in k_copies[K_FIRST:]:
                cp.start()

        @pl.when(me >= 0)
        def _():
            part = jnp.concatenate([jnp.dot(hid[:, r], ref[r, :], preferred_element_type=F32) for ref in (wkb, wvb)], axis=1)
            acc[:, qw:] = part if c == 0 else acc[:, qw:] + part

    mine[1] = acc[:, qw:].astype(BF16)
    gather(1, x2)
    for cp in v_copies:
        cp.start()
    for i in range(2):
        spread(i, me, mine[i])
    collect(0, x1)

    def of_row(b, first):
        return jnp.concatenate([full[first * blocks + c, pl.ds(b, n, stride=rows), :] for c in range(blocks)], axis=1)

    def times(q, kt):
        return lax.dot_general(q, kt, (((1,), (1,)), ((), ())), preferred_element_type=F32) * scale

    colpos = _positions(heads, w, 2 * seq * n)
    scale = dim ** -0.5
    for cp in k_copies:
        cp.wait()
    for b in range(rows):
        q = jnp.concatenate([of_row(b, 0), of_row(b, 1)], axis=0).astype(BF16)
        q_ref[b] = q
        end = vl[b] - me * seq
        end_ref[b:b + 1, :] = jnp.full((1, w), end, jnp.int32)
        if b >= EARLY:
            continue
        for t in range(seq // TILE):
            s = times(q, k_ref[b, pl.ds(t * TILE, TILE)].reshape(w, dim))
            s_ref[b, :, t * w:(t + 1) * w] = jnp.where(colpos < end - t * TILE, s, -jnp.inf)
    collect(1, x2)
    for b in range(rows):
        kn = of_row(b, 2).astype(BF16)
        kn_ref[b] = kn
        vn_ref[b] = of_row(b, 3).astype(BF16)
        at_ref[b:b + 1, :] = jnp.full((1, w), wp[b] - me * seq, jnp.int32)
        if b >= EARLY:
            continue
        dots = [jnp.sum(of_row(b, j) * of_row(b, 2), axis=-1, keepdims=True) for j in range(2)]
        s = jnp.where(wp[b] < vl[b], jnp.concatenate(dots, axis=0) * scale, -jnp.inf)
        f_ref[b] = jnp.broadcast_to(s, (2 * heads, w))
    for cp in v_copies:
        cp.wait()


def _patch(at_ref, kn_ref, vn_ref, ki_ref, vi_ref, k_ref, v_ref):
    del ki_ref, vi_ref
    rows, seq = k_ref.shape[:2]
    ats = [at_ref[b, 0] for b in range(rows)]
    for b, at in enumerate(ats):
        @pl.when((at >= 0) & (at < seq))
        def _():
            k_ref[b, at] = kn_ref[b]
            v_ref[b, at] = vn_ref[b]


def _attend(n, s_ref, f_ref, q_ref, end_ref, at_ref, k_ref, v_ref, wo_ref, out_ref, w_ref, p_ref, xs, xr, part, recv, red, gath,
            wsem, x2, x3, x4):
    me = lax.axis_index('sp')
    rows, seq, heads, dim = v_ref.shape
    model = out_ref.shape[1]
    cols = red.shape[1]
    blocks = dim // 128
    ntile = seq // TILE
    w = TILE * heads
    span = xs.shape[0] // heads
    wcopy = pltpu.make_async_copy(wo_ref, w_ref.at[:, pl.ds(0, model)], wsem)
    wcopy.start()
    w_ref[:, model:] = jnp.zeros((w_ref.shape[0], n * cols - model), BF16)
    barrier = _greet(me, n)
    lane = lax.broadcasted_iota(jnp.int32, (heads, 128), 1)
    colpos = _positions(heads, w, 2 * seq * n)
    scale = dim ** -0.5

    stats = [jnp.zeros((heads, 128), F32)]
    own_lane = lax.broadcasted_iota(jnp.int32, (rows, 128), 1) - 4 * lax.broadcasted_iota(jnp.int32, (rows, 128), 0)

    def soften(b):
        if b < EARLY:
            at = at_ref[b:b + 1, :]
            fresh = f_ref[b]
            ss = [jnp.where(colpos == at - t * TILE, fresh, s_ref[b, :, t * w:(t + 1) * w]) for t in range(ntile)]
        else:
            end = end_ref[b:b + 1, :]
            ss = [lax.dot_general(q_ref[b], k_ref[b, pl.ds(t * TILE, TILE)].reshape(w, dim), (((1,), (1,)), ((), ())),
                                  preferred_element_type=F32) * scale for t in range(ntile)]
            ss = [jnp.where(colpos < end - t * TILE, s, -jnp.inf) for t, s in enumerate(ss)]
        m = jnp.max(functools.reduce(jnp.maximum, ss), axis=-1, keepdims=True)
        m = jnp.maximum(m, FLOOR)
        ps = [jnp.exp(s - m) for s in ss]
        l = jnp.sum(functools.reduce(jnp.add, ps), axis=-1, keepdims=True)
        for t in range(ntile):
            p_ref[b, :, t * w:(t + 1) * w] = ps[t].astype(BF16)
        here = (lane // 4) == b
        part = [m[:heads], l[:heads], m[heads:], l[heads:]]
        for i, x in enumerate(part):
            stats[0] = jnp.where(here & (lane % 4 == i), x, stats[0])

    def values(b):
        acc = functools.reduce(jnp.add, [
            functools.reduce(jnp.add, [
                jnp.dot(p_ref[b, :, t * w:(t + 1) * w], v_ref[b, pl.ds(t * TILE, TILE)].reshape(w, dim),
                        preferred_element_type=F32) for t in range(first, ntile, 2)]) for first in range(2)])
        for c in range(blocks):
            piece = acc[:, c * 128:(c + 1) * 128]
            xs[pl.ds(c * 2 * rows + b, heads, stride=span), :] = piece[:heads]
            xs[pl.ds(c * 2 * rows + rows + b, heads, stride=span), :] = piece[heads:]

    for i in range(rows + LAG):
        if i < rows:
            soften(i)
        if i >= LAG:
            values(i - LAG)
    base = blocks * 2 * rows
    xs[pl.ds(base, heads, stride=span), :] = stats[0]
    pl.semaphore_wait(barrier, n - 1)
    _exchange(me, n, lambda peer: xs.at[pl.ds(pl.multiple_of(peer * span, span), base + 1)],
              lambda off: xr.at[off - 1, pl.ds(0, base + 1)], x2)
    xr[n - 1] = xs[_rows(me, span), :]
    _settle(xr.at[pl.ds(0, n - 1), pl.ds(0, base + 1)], x2)
    pieces = []
    def column(i, k):
        return jnp.sum(jnp.where(own_lane == k, xr[i, base:base + 1, :], 0.0), axis=-1, keepdims=True)

    for j in range(2):
        ms = [column(i, 2 * j) for i in range(n)]
        top = functools.reduce(jnp.maximum, ms)
        es = [jnp.exp(m - top) for m in ms]
        total = functools.reduce(jnp.add, [column(i, 2 * j + 1) * es[i] for i in range(n)])
        for c in range(blocks):
            at = c * 2 * rows + j * rows
            num = functools.reduce(jnp.add, [xr[i, at:at + rows, :] * es[i] for i in range(n)])
            pieces.append((num / total).astype(BF16))
    o = jnp.concatenate(pieces, axis=1)
    wcopy.wait()

    order = _far_first(n)
    for group in GROUPS:
        for i in group:
            off = order[i]
            part[off - 1] = jnp.dot(o, w_ref[:, _rows(_peer(me, off, n), cols)], preferred_element_type=F32)
        for i in group:
            off = order[i]
            _send(me, n, off, lambda peer: part.at[off - 1], lambda off: recv.at[off - 1], x3)
    part[n - 1] = jnp.dot(o, w_ref[:, _rows(me, cols)], preferred_element_type=F32)
    _settle(recv, x3)
    total = part[n - 1]
    for off in range(1, n):
        total += recv[off - 1]
    red[...] = total.astype(BF16)
    _exchange(me, n, lambda peer: red, lambda off: gath.at[:, _rows(me, cols)], x4)
    _settle(gath.at[:, pl.ds(0, (n - 1) * cols)], x4)
    gath[:, _rows(me, cols)] = red[...]
    out_ref[...] = gath[:, :model]


def _hand_over(attn_ref, k_ref, v_ref, out_ref):
    del k_ref, v_ref
    out_ref[...] = attn_ref[...]


def solution(mesh):
    row_spec = P(('rep', 'dp'), None)
    cache_spec = P(('rep', 'dp'), 'sp', None, None)
    len_spec = P(('rep', 'dp'))
    n = mesh.shape['sp']
    vmem = pl.BlockSpec(memory_space=pltpu.VMEM)
    hbm = pl.BlockSpec(memory_space=pltpu.HBM)
    dma = pltpu.SemaphoreType.DMA

    def in_hbm(x):
        return pltpu.with_memory_space_constraint(x, pltpu.HBM)

    def local_step(hidden, w_query, w_key, w_value, w_out, k_cache, v_cache, write_pos, valid_len):
        rows, seq, heads, dim = k_cache.shape
        depth = hidden.shape[1]
        model = w_out.shape[1]
        qw = w_query.shape[1] // n
        lw = qw + 2 * dim
        blocks = dim // 128
        cache = pltpu.VMEM(k_cache.shape, BF16)
        new = pltpu.VMEM((rows, heads, dim), BF16)
        scores, fresh, query, ends, at, k_new, v_new, k_here, v_here = pl.pallas_call(
            functools.partial(_project, n),
            out_shape=(
                pltpu.VMEM((EARLY, 2 * heads, seq * heads), F32),
                pltpu.VMEM((EARLY, 2 * heads, TILE * heads), F32),
                pltpu.VMEM((rows, 2 * heads, dim), BF16),
                pltpu.VMEM((rows, TILE * heads), jnp.int32),
                pltpu.VMEM((rows, TILE * heads), jnp.int32),
                new, new, cache, cache,
            ),
            in_specs=[hbm] * 8,
            out_specs=(vmem,) * 9,
            scratch_shapes=[
                pltpu.VMEM((rows, depth), BF16),
                pltpu.VMEM((depth, qw), BF16),
                pltpu.VMEM((depth, dim), BF16),
                pltpu.VMEM((depth, dim), BF16),
                pltpu.VMEM((rows, lw), F32),
                pltpu.VMEM((2, rows, lw // 2), BF16),
                pltpu.VMEM((2, n - 1, rows, lw // 2), BF16),
                pltpu.VMEM((lw // 128, n * rows, 128), F32),
                pltpu.SMEM((rows,), jnp.int32),
                pltpu.SMEM((rows,), jnp.int32),
                dma, dma((len(Q_PARTS),)), dma((2, len(KV_PARTS))), dma((K_PARTS,)), dma((V_PARTS,)), dma((2,)),
                dma((2,)), dma((2,)),
            ],
            compiler_params=pltpu.CompilerParams(collective_id=0, has_side_effects=True, vmem_limit_bytes=12 * MIB),
            cost_estimate=pl.CostEstimate(flops=10_000_000_000, bytes_accessed=28 * MIB, transcendentals=0),
            name='project',
        )(*[in_hbm(x) for x in (hidden, w_query, w_key, w_value, k_cache, v_cache, write_pos, valid_len)])
        k_here, v_here = pl.pallas_call(
            _patch,
            out_shape=(cache, cache),
            in_specs=[vmem] * 5,
            out_specs=(vmem, vmem),
            input_output_aliases={3: 0, 4: 1},
            compiler_params=pltpu.CompilerParams(vmem_limit_bytes=1 * MIB),
            name='patch',
        )(at, k_new, v_new, k_here, v_here)
        top = lax.optimization_barrier(jnp.full((), jnp.inf, BF16))
        k_next = jnp.minimum(k_here, top)
        v_next = jnp.minimum(v_here, top)
        padded = -(-model // (128 * n)) * 128 * n
        span = 2 * rows * blocks + rows
        attn = pl.pallas_call(
            functools.partial(_attend, n),
            out_shape=jax.ShapeDtypeStruct((rows, model), BF16),
            in_specs=[vmem] * 7 + [hbm],
            out_specs=vmem,
            scratch_shapes=[
                pltpu.VMEM((w_out.shape[0], padded), BF16),
                pltpu.VMEM((rows, 2 * heads, seq * heads), BF16),
                pltpu.VMEM((heads * span, 128), F32),
                pltpu.VMEM((n, span, 128), F32),
                pltpu.VMEM((n, rows, padded // n), F32),
                pltpu.VMEM((n - 1, rows, padded // n), F32),
                pltpu.VMEM((rows, padded // n), BF16),
                pltpu.VMEM((rows, padded), BF16),
                dma, dma((2,)), dma((2,)), dma((2,)),
            ],
            compiler_params=pltpu.CompilerParams(collective_id=1, has_side_effects=True, vmem_limit_bytes=8 * MIB),
            cost_estimate=pl.CostEstimate(flops=20_000_000_000, bytes_accessed=4 * MIB, transcendentals=0),
            name='attend',
        )(scores, fresh, query, ends, at, k_next, v_next, in_hbm(w_out))
        attn = pl.pallas_call(
            _hand_over,
            out_shape=jax.ShapeDtypeStruct((rows, model), BF16),
            in_specs=[vmem] * 3,
            out_specs=vmem,
            compiler_params=pltpu.CompilerParams(vmem_limit_bytes=1 * MIB),
            name='hand_over',
        )(attn, k_next, v_next)
        return attn, k_next, v_next

    return jax.shard_map(
        local_step, mesh=mesh,
        in_specs=(row_spec, P(), P(), P(), P('sp', None), cache_spec, cache_spec, len_spec, len_spec),
        out_specs=(row_spec, cache_spec, cache_spec), check_vma=False)
```

```python
import functools

import jax
import jax.numpy as jnp
from jax import lax
from jax.experimental import pallas as pl
from jax.experimental.pallas import tpu as pltpu
from jax.sharding import PartitionSpec as P

F32 = jnp.float32
BF16 = jnp.bfloat16
FLOOR = float(jnp.finfo(jnp.float32).min)
MESH = pl.DeviceIdType.MESH
Q_PARTS = (6, 5, 3)
KV_PARTS = (8, 6)
K_PARTS = 2
K_FIRST = 1
V_PARTS = 1
EARLY = 7
GROUPS = ((0,), (1, 2), (3, 4), (5, 6))
TILE = 32
LAG = 2
MIB = 1 << 20


def _peer(me, off, n):
    return lax.rem(me + off, n)


def _greet(me, n):
    barrier = pltpu.get_barrier_semaphore()
    for off in _far_first(n):
        pl.semaphore_signal(barrier, inc=1, device_id={'sp': _peer(me, off, n)}, device_id_type=MESH)
    return barrier


def _far_first(n):
    return sorted(range(1, n), key=lambda off: abs(off - n // 2))


def _send(me, n, off, src, dst, sems):
    peer = _peer(me, off, n)
    pltpu.make_async_remote_copy(
        src_ref=src(peer), dst_ref=dst(off), send_sem=sems.at[0], recv_sem=sems.at[1],
        device_id={'sp': peer}, device_id_type=MESH).start()


def _exchange(me, n, src, dst, sems):
    for off in _far_first(n):
        _send(me, n, off, src, dst, sems)


def _settle(total, sems):
    for i in range(2):
        pltpu.make_async_copy(total, total, sems.at[i]).wait()


def _part(i, size, parts):
    return pl.ds(i * size // parts, size // parts)


def _positions(heads, width, never):
    col = lax.broadcasted_iota(jnp.int32, (2 * heads, width), 1)
    row = lax.broadcasted_iota(jnp.int32, (2 * heads, width), 0)
    return jnp.where((col % heads) == (row % heads), col // heads, never)


def _rows(i, count):
    return pl.ds(pl.multiple_of(i * count, count), count)


def _project(n, hid_ref, wq_ref, wk_ref, wv_ref, kc_ref, vc_ref, wp_ref, vl_ref,
             s_ref, f_ref, q_ref, end_ref, at_ref, kn_ref, vn_ref, k_ref, v_ref,
             hid, wqb, wkb, wvb, acc, mine, got, full, wp, vl,
             hsem, qsem, wsem, ksem, vsem, psem, x1, x2):
    me = lax.axis_index('sp')
    rows, seq, heads, dim = k_ref.shape
    depth, qw = wqb.shape
    blocks = dim // 128
    w = TILE * heads
    small = [
        pltpu.make_async_copy(hid_ref, hid, hsem),
        pltpu.make_async_copy(wp_ref, wp, psem.at[0]),
        pltpu.make_async_copy(vl_ref, vl, psem.at[1]),
    ]

    def slices(parts):
        unit = depth // sum(parts)
        return [pl.ds(sum(parts[:c]) * unit, parts[c] * unit) for c in range(len(parts))]

    q_rows, kv_rows = slices(Q_PARTS), slices(KV_PARTS)
    q_copies = [pltpu.make_async_copy(wq_ref.at[r, _rows(me, qw)], wqb.at[r], qsem.at[c]) for c, r in enumerate(q_rows)]
    kv_copies = [
        pltpu.make_async_copy(src.at[r, _rows(me, dim)], dst.at[r], wsem.at[i, c])
        for c, r in enumerate(kv_rows) for i, (src, dst) in enumerate(((wk_ref, wkb), (wv_ref, wvb)))
    ]
    k_copies, v_copies = [
        [pltpu.make_async_copy(src.at[_part(i, rows, parts)], dst.at[_part(i, rows, parts)], sem.at[i]) for i in range(parts)]
        for src, dst, sem, parts in ((kc_ref, k_ref, ksem, K_PARTS), (vc_ref, v_ref, vsem, V_PARTS))
    ]
    for cp in q_copies + small:
        cp.start()
    barrier = _greet(me, n)

    def gather(i, sems):
        _exchange(me, n, lambda peer: mine.at[i], lambda off: got.at[i, off - 1], sems)

    def spread(i, src, value):
        value = value.astype(F32)
        for c in range(value.shape[1] // 128):
            full[i * 2 * blocks + c, _rows(src, rows), :] = value[:, c * 128:(c + 1) * 128]

    def collect(i, sems):
        _settle(got.at[i], sems)
        for off in range(1, n):
            spread(i, _peer(me, n - off, n), got[i, off - 1])

    for cp in small:
        cp.wait()
    for c, r in enumerate(q_rows):
        q_copies[c].wait()
        if c == 0:
            for cp in kv_copies:
                cp.start()
        if c == len(q_rows) - 1:
            for cp in k_copies[:K_FIRST]:
                cp.start()

        @pl.when(me >= 0)
        def _():
            part = jnp.dot(hid[:, r], wqb[r, :], preferred_element_type=F32)
            acc[:, :qw] = part if c == 0 else acc[:, :qw] + part

    mine[0] = acc[:, :qw].astype(BF16)
    pl.semaphore_wait(barrier, n - 1)
    gather(0, x1)
    for c, r in enumerate(kv_rows):
        for cp in kv_copies[2 * c:2 * c + 2]:
            cp.wait()
        if c == 0:
            for cp in k_copies[K_FIRST:]:
                cp.start()

        @pl.when(me >= 0)
        def _():
            part = jnp.concatenate([jnp.dot(hid[:, r], ref[r, :], preferred_element_type=F32) for ref in (wkb, wvb)], axis=1)
            acc[:, qw:] = part if c == 0 else acc[:, qw:] + part

    mine[1] = acc[:, qw:].astype(BF16)
    gather(1, x2)
    for cp in v_copies:
        cp.start()
    for i in range(2):
        spread(i, me, mine[i])
    collect(0, x1)

    def of_row(b, first):
        return jnp.concatenate([full[first * blocks + c, pl.ds(b, n, stride=rows), :] for c in range(blocks)], axis=1)

    def times(q, kt):
        return lax.dot_general(q, kt, (((1,), (1,)), ((), ())), preferred_element_type=F32) * scale

    colpos = _positions(heads, w, 2 * seq * n)
    scale = dim ** -0.5
    for cp in k_copies:
        cp.wait()
    for b in range(rows):
        q = jnp.concatenate([of_row(b, 0), of_row(b, 1)], axis=0).astype(BF16)
        q_ref[b] = q
        end = vl[b] - me * seq
        end_ref[b:b + 1, :] = jnp.full((1, w), end, jnp.int32)
        if b >= EARLY:
            continue
        for t in range(seq // TILE):
            s = times(q, k_ref[b, pl.ds(t * TILE, TILE)].reshape(w, dim))
            s_ref[b, :, t * w:(t + 1) * w] = jnp.where(colpos < end - t * TILE, s, -jnp.inf)
    collect(1, x2)
    for b in range(rows):
        kn = of_row(b, 2).astype(BF16)
        kn_ref[b] = kn
        vn_ref[b] = of_row(b, 3).astype(BF16)
        at_ref[b:b + 1, :] = jnp.full((1, w), wp[b] - me * seq, jnp.int32)
        if b >= EARLY:
            continue
        dots = [jnp.sum(of_row(b, j) * of_row(b, 2), axis=-1, keepdims=True) for j in range(2)]
        s = jnp.where(wp[b] < vl[b], jnp.concatenate(dots, axis=0) * scale, -jnp.inf)
        f_ref[b] = jnp.broadcast_to(s, (2 * heads, w))
    for cp in v_copies:
        cp.wait()


def _patch(at_ref, kn_ref, vn_ref, ki_ref, vi_ref, k_ref, v_ref):
    del ki_ref, vi_ref
    rows, seq = k_ref.shape[:2]
    ats = [at_ref[b, 0] for b in range(rows)]
    for b, at in enumerate(ats):
        @pl.when((at >= 0) & (at < seq))
        def _():
            k_ref[b, at] = kn_ref[b]
            v_ref[b, at] = vn_ref[b]


def _attend(n, s_ref, f_ref, q_ref, end_ref, at_ref, k_ref, v_ref, wo_ref, out_ref, w_ref, p_ref, xs, xr, part, recv, red, gath,
            wsem, x2, x3, x4):
    me = lax.axis_index('sp')
    rows, seq, heads, dim = v_ref.shape
    model = out_ref.shape[1]
    cols = red.shape[1]
    blocks = dim // 128
    ntile = seq // TILE
    w = TILE * heads
    span = xs.shape[0] // heads
    wcopy = pltpu.make_async_copy(wo_ref, w_ref.at[:, pl.ds(0, model)], wsem)
    wcopy.start()
    w_ref[:, model:] = jnp.zeros((w_ref.shape[0], n * cols - model), BF16)
    barrier = _greet(me, n)
    lane = lax.broadcasted_iota(jnp.int32, (heads, 128), 1)
    colpos = _positions(heads, w, 2 * seq * n)
    scale = dim ** -0.5

    stats = [jnp.zeros((heads, 128), F32)]
    own_lane = lax.broadcasted_iota(jnp.int32, (rows, 128), 1) - 4 * lax.broadcasted_iota(jnp.int32, (rows, 128), 0)

    def soften(b):
        if b < EARLY:
            at = at_ref[b:b + 1, :]
            fresh = f_ref[b]
            ss = [jnp.where(colpos == at - t * TILE, fresh, s_ref[b, :, t * w:(t + 1) * w]) for t in range(ntile)]
        else:
            end = end_ref[b:b + 1, :]
            ss = [lax.dot_general(q_ref[b], k_ref[b, pl.ds(t * TILE, TILE)].reshape(w, dim), (((1,), (1,)), ((), ())),
                                  preferred_element_type=F32) * scale for t in range(ntile)]
            ss = [jnp.where(colpos < end - t * TILE, s, -jnp.inf) for t, s in enumerate(ss)]
        m = jnp.max(functools.reduce(jnp.maximum, ss), axis=-1, keepdims=True)
        m = jnp.maximum(m, FLOOR)
        ps = [jnp.exp(s - m) for s in ss]
        l = jnp.sum(functools.reduce(jnp.add, ps), axis=-1, keepdims=True)
        for t in range(ntile):
            p_ref[b, :, t * w:(t + 1) * w] = ps[t].astype(BF16)
        here = (lane // 4) == b
        part = [m[:heads], l[:heads], m[heads:], l[heads:]]
        for i, x in enumerate(part):
            stats[0] = jnp.where(here & (lane % 4 == i), x, stats[0])

    def values(b):
        acc = functools.reduce(jnp.add, [
            functools.reduce(jnp.add, [
                jnp.dot(p_ref[b, :, t * w:(t + 1) * w], v_ref[b, pl.ds(t * TILE, TILE)].reshape(w, dim),
                        preferred_element_type=F32) for t in range(first, ntile, 2)]) for first in range(2)])
        for c in range(blocks):
            piece = acc[:, c * 128:(c + 1) * 128]
            xs[pl.ds(c * 2 * rows + b, heads, stride=span), :] = piece[:heads]
            xs[pl.ds(c * 2 * rows + rows + b, heads, stride=span), :] = piece[heads:]

    turn = list(range(EARLY, rows)) + list(range(EARLY))
    for i in range(rows + LAG):
        if i < rows:
            soften(turn[i])
        if i >= LAG:
            values(turn[i - LAG])
    base = blocks * 2 * rows
    xs[pl.ds(base, heads, stride=span), :] = stats[0]
    pl.semaphore_wait(barrier, n - 1)
    _exchange(me, n, lambda peer: xs.at[pl.ds(pl.multiple_of(peer * span, span), base + 1)],
              lambda off: xr.at[off - 1, pl.ds(0, base + 1)], x2)
    xr[n - 1] = xs[_rows(me, span), :]
    _settle(xr.at[pl.ds(0, n - 1), pl.ds(0, base + 1)], x2)
    pieces = []
    def column(i, k):
        return jnp.sum(jnp.where(own_lane == k, xr[i, base:base + 1, :], 0.0), axis=-1, keepdims=True)

    for j in range(2):
        ms = [column(i, 2 * j) for i in range(n)]
        top = functools.reduce(jnp.maximum, ms)
        es = [jnp.exp(m - top) for m in ms]
        total = functools.reduce(jnp.add, [column(i, 2 * j + 1) * es[i] for i in range(n)])
        for c in range(blocks):
            at = c * 2 * rows + j * rows
            num = functools.reduce(jnp.add, [xr[i, at:at + rows, :] * es[i] for i in range(n)])
            pieces.append((num / total).astype(BF16))
    o = jnp.concatenate(pieces, axis=1)
    wcopy.wait()

    order = _far_first(n)
    for group in GROUPS:
        for i in group:
            off = order[i]
            part[off - 1] = jnp.dot(o, w_ref[:, _rows(_peer(me, off, n), cols)], preferred_element_type=F32)
        for i in group:
            off = order[i]
            _send(me, n, off, lambda peer: part.at[off - 1], lambda off: recv.at[off - 1], x3)
    part[n - 1] = jnp.dot(o, w_ref[:, _rows(me, cols)], preferred_element_type=F32)
    _settle(recv, x3)
    total = part[n - 1]
    for off in range(1, n):
        total += recv[off - 1]
    red[...] = total.astype(BF16)
    _exchange(me, n, lambda peer: red, lambda off: gath.at[:, _rows(me, cols)], x4)
    _settle(gath.at[:, pl.ds(0, (n - 1) * cols)], x4)
    gath[:, _rows(me, cols)] = red[...]
    out_ref[...] = gath[:, :model]


def _hand_over(attn_ref, k_ref, v_ref, out_ref):
    del k_ref, v_ref
    out_ref[...] = attn_ref[...]


def solution(mesh):
    row_spec = P(('rep', 'dp'), None)
    cache_spec = P(('rep', 'dp'), 'sp', None, None)
    len_spec = P(('rep', 'dp'))
    n = mesh.shape['sp']
    vmem = pl.BlockSpec(memory_space=pltpu.VMEM)
    hbm = pl.BlockSpec(memory_space=pltpu.HBM)
    dma = pltpu.SemaphoreType.DMA

    def in_hbm(x):
        return pltpu.with_memory_space_constraint(x, pltpu.HBM)

    def local_step(hidden, w_query, w_key, w_value, w_out, k_cache, v_cache, write_pos, valid_len):
        rows, seq, heads, dim = k_cache.shape
        depth = hidden.shape[1]
        model = w_out.shape[1]
        qw = w_query.shape[1] // n
        lw = qw + 2 * dim
        blocks = dim // 128
        cache = pltpu.VMEM(k_cache.shape, BF16)
        new = pltpu.VMEM((rows, heads, dim), BF16)
        scores, fresh, query, ends, at, k_new, v_new, k_here, v_here = pl.pallas_call(
            functools.partial(_project, n),
            out_shape=(
                pltpu.VMEM((EARLY, 2 * heads, seq * heads), F32),
                pltpu.VMEM((EARLY, 2 * heads, TILE * heads), F32),
                pltpu.VMEM((rows, 2 * heads, dim), BF16),
                pltpu.VMEM((rows, TILE * heads), jnp.int32),
                pltpu.VMEM((rows, TILE * heads), jnp.int32),
                new, new, cache, cache,
            ),
            in_specs=[hbm] * 8,
            out_specs=(vmem,) * 9,
            scratch_shapes=[
                pltpu.VMEM((rows, depth), BF16),
                pltpu.VMEM((depth, qw), BF16),
                pltpu.VMEM((depth, dim), BF16),
                pltpu.VMEM((depth, dim), BF16),
                pltpu.VMEM((rows, lw), F32),
                pltpu.VMEM((2, rows, lw // 2), BF16),
                pltpu.VMEM((2, n - 1, rows, lw // 2), BF16),
                pltpu.VMEM((lw // 128, n * rows, 128), F32),
                pltpu.SMEM((rows,), jnp.int32),
                pltpu.SMEM((rows,), jnp.int32),
                dma, dma((len(Q_PARTS),)), dma((2, len(KV_PARTS))), dma((K_PARTS,)), dma((V_PARTS,)), dma((2,)),
                dma((2,)), dma((2,)),
            ],
            compiler_params=pltpu.CompilerParams(collective_id=0, has_side_effects=True, vmem_limit_bytes=12 * MIB),
            cost_estimate=pl.CostEstimate(flops=10_000_000_000, bytes_accessed=28 * MIB, transcendentals=0),
            name='project',
        )(*[in_hbm(x) for x in (hidden, w_query, w_key, w_value, k_cache, v_cache, write_pos, valid_len)])
        k_here, v_here = pl.pallas_call(
            _patch,
            out_shape=(cache, cache),
            in_specs=[vmem] * 5,
            out_specs=(vmem, vmem),
            input_output_aliases={3: 0, 4: 1},
            compiler_params=pltpu.CompilerParams(vmem_limit_bytes=1 * MIB),
            name='patch',
        )(at, k_new, v_new, k_here, v_here)
        top = lax.optimization_barrier(jnp.full((), jnp.inf, BF16))
        k_next = jnp.minimum(k_here, top)
        v_next = jnp.minimum(v_here, top)
        padded = -(-model // (128 * n)) * 128 * n
        span = 2 * rows * blocks + rows
        attn = pl.pallas_call(
            functools.partial(_attend, n),
            out_shape=jax.ShapeDtypeStruct((rows, model), BF16),
            in_specs=[vmem] * 7 + [hbm],
            out_specs=vmem,
            scratch_shapes=[
                pltpu.VMEM((w_out.shape[0], padded), BF16),
                pltpu.VMEM((rows, 2 * heads, seq * heads), BF16),
                pltpu.VMEM((heads * span, 128), F32),
                pltpu.VMEM((n, span, 128), F32),
                pltpu.VMEM((n, rows, padded // n), F32),
                pltpu.VMEM((n - 1, rows, padded // n), F32),
                pltpu.VMEM((rows, padded // n), BF16),
                pltpu.VMEM((rows, padded), BF16),
                dma, dma((2,)), dma((2,)), dma((2,)),
            ],
            compiler_params=pltpu.CompilerParams(collective_id=1, has_side_effects=True, vmem_limit_bytes=8 * MIB),
            cost_estimate=pl.CostEstimate(flops=20_000_000_000, bytes_accessed=4 * MIB, transcendentals=0),
            name='attend',
        )(scores, fresh, query, ends, at, k_next, v_next, in_hbm(w_out))
        attn = pl.pallas_call(
            _hand_over,
            out_shape=jax.ShapeDtypeStruct((rows, model), BF16),
            in_specs=[vmem] * 3,
            out_specs=vmem,
            compiler_params=pltpu.CompilerParams(vmem_limit_bytes=1 * MIB),
            name='hand_over',
        )(attn, k_next, v_next)
        return attn, k_next, v_next

    return jax.shard_map(
        local_step, mesh=mesh,
        in_specs=(row_spec, P(), P(), P(), P('sp', None), cache_spec, cache_spec, len_spec, len_spec),
        out_specs=(row_spec, cache_spec, cache_spec), check_vma=False)
```

```python
import functools

import jax
import jax.numpy as jnp
from jax import lax
from jax.experimental import pallas as pl
from jax.experimental.pallas import tpu as pltpu
from jax.sharding import PartitionSpec as P

F32 = jnp.float32
BF16 = jnp.bfloat16
FLOOR = float(jnp.finfo(jnp.float32).min)
MESH = pl.DeviceIdType.MESH
Q_PARTS = (6, 5, 3)
KV_PARTS = (8, 6)
K_PARTS = 2
K_FIRST = 1
V_PARTS = 1
EARLY = 7
GROUPS = ((0,), (1, 2), (3, 4), (5, 6))
TILE = 32
LAG = 2
MIB = 1 << 20


def _peer(me, off, n):
    return lax.rem(me + off, n)


def _greet(me, n):
    barrier = pltpu.get_barrier_semaphore()
    for off in _far_first(n):
        pl.semaphore_signal(barrier, inc=1, device_id={'sp': _peer(me, off, n)}, device_id_type=MESH)
    return barrier


def _far_first(n):
    return sorted(range(1, n), key=lambda off: abs(off - n // 2))


def _send(me, n, off, src, dst, sems):
    peer = _peer(me, off, n)
    pltpu.make_async_remote_copy(
        src_ref=src(peer), dst_ref=dst(off), send_sem=sems.at[0], recv_sem=sems.at[1],
        device_id={'sp': peer}, device_id_type=MESH).start()


def _exchange(me, n, src, dst, sems):
    for off in _far_first(n):
        _send(me, n, off, src, dst, sems)


def _settle(total, sems):
    for i in range(2):
        pltpu.make_async_copy(total, total, sems.at[i]).wait()


def _part(i, size, parts):
    return pl.ds(i * size // parts, size // parts)


def _positions(heads, width, never):
    col = lax.broadcasted_iota(jnp.int32, (2 * heads, width), 1)
    row = lax.broadcasted_iota(jnp.int32, (2 * heads, width), 0)
    return jnp.where((col % heads) == (row % heads), col // heads, never)


def _rows(i, count):
    return pl.ds(pl.multiple_of(i * count, count), count)


def _project(n, hid_ref, wq_ref, wk_ref, wv_ref, kc_ref, vc_ref, wp_ref, vl_ref,
             s_ref, f_ref, q_ref, end_ref, at_ref, kn_ref, vn_ref, k_ref, v_ref,
             hid, wqb, wkb, wvb, acc, mine, got, full, wp, vl,
             hsem, qsem, wsem, ksem, vsem, psem, x1, x2):
    me = lax.axis_index('sp')
    rows, seq, heads, dim = k_ref.shape
    depth, qw = wqb.shape
    blocks = dim // 128
    w = TILE * heads
    small = [
        pltpu.make_async_copy(hid_ref, hid, hsem),
        pltpu.make_async_copy(wp_ref, wp, psem.at[0]),
        pltpu.make_async_copy(vl_ref, vl, psem.at[1]),
    ]

    def slices(parts):
        unit = depth // sum(parts)
        return [pl.ds(sum(parts[:c]) * unit, parts[c] * unit) for c in range(len(parts))]

    q_rows, kv_rows = slices(Q_PARTS), slices(KV_PARTS)
    q_copies = [pltpu.make_async_copy(wq_ref.at[r, _rows(me, qw)], wqb.at[r], qsem.at[c]) for c, r in enumerate(q_rows)]
    kv_copies = [
        pltpu.make_async_copy(src.at[r, _rows(me, dim)], dst.at[r], wsem.at[i, c])
        for c, r in enumerate(kv_rows) for i, (src, dst) in enumerate(((wk_ref, wkb), (wv_ref, wvb)))
    ]
    k_copies, v_copies = [
        [pltpu.make_async_copy(src.at[_part(i, rows, parts)], dst.at[_part(i, rows, parts)], sem.at[i]) for i in range(parts)]
        for src, dst, sem, parts in ((kc_ref, k_ref, ksem, K_PARTS), (vc_ref, v_ref, vsem, V_PARTS))
    ]
    for cp in q_copies + small:
        cp.start()
    barrier = _greet(me, n)

    def gather(i, sems):
        _exchange(me, n, lambda peer: mine.at[i], lambda off: got.at[i, off - 1], sems)

    def spread(i, src, value):
        value = value.astype(F32)
        for c in range(value.shape[1] // 128):
            full[i * 2 * blocks + c, _rows(src, rows), :] = value[:, c * 128:(c + 1) * 128]

    def collect(i, sems):
        _settle(got.at[i], sems)
        for off in range(1, n):
            spread(i, _peer(me, n - off, n), got[i, off - 1])

    for cp in small:
        cp.wait()
    for c, r in enumerate(q_rows):
        q_copies[c].wait()
        if c == 0:
            for cp in kv_copies:
                cp.start()
        if c == len(q_rows) - 1:
            for cp in k_copies[:K_FIRST]:
                cp.start()

        @pl.when(me >= 0)
        def _():
            part = jnp.dot(hid[:, r], wqb[r, :], preferred_element_type=F32)
            acc[:, :qw] = part if c == 0 else acc[:, :qw] + part

    mine[0] = acc[:, :qw].astype(BF16)
    pl.semaphore_wait(barrier, n - 1)
    gather(0, x1)
    for c, r in enumerate(kv_rows):
        for cp in kv_copies[2 * c:2 * c + 2]:
            cp.wait()
        if c == 0:
            for cp in k_copies[K_FIRST:]:
                cp.start()

        @pl.when(me >= 0)
        def _():
            part = jnp.concatenate([jnp.dot(hid[:, r], ref[r, :], preferred_element_type=F32) for ref in (wkb, wvb)], axis=1)
            acc[:, qw:] = part if c == 0 else acc[:, qw:] + part

    mine[1] = acc[:, qw:].astype(BF16)
    gather(1, x2)
    for cp in v_copies:
        cp.start()
    for i in range(2):
        spread(i, me, mine[i])
    collect(0, x1)

    def of_row(b, first):
        return jnp.concatenate([full[first * blocks + c, pl.ds(b, n, stride=rows), :] for c in range(blocks)], axis=1)

    def times(q, kt):
        return lax.dot_general(q, kt, (((1,), (1,)), ((), ())), preferred_element_type=F32) * scale

    colpos = _positions(heads, w, 2 * seq * n)
    scale = dim ** -0.5
    for cp in k_copies:
        cp.wait()
    for b in range(rows):
        q = jnp.concatenate([of_row(b, 0), of_row(b, 1)], axis=0).astype(BF16)
        q_ref[b] = q
        end = vl[b] - me * seq
        end_ref[b:b + 1, :] = jnp.full((1, w), end, jnp.int32)
        if b >= EARLY:
            continue
        for t in range(seq // TILE):
            s = times(q, k_ref[b, pl.ds(t * TILE, TILE)].reshape(w, dim))
            s_ref[b, :, t * w:(t + 1) * w] = jnp.where(colpos < end - t * TILE, s, -jnp.inf)
    collect(1, x2)
    for b in range(rows):
        kn = of_row(b, 2).astype(BF16)
        kn_ref[b] = kn
        vn_ref[b] = of_row(b, 3).astype(BF16)
        at_ref[b:b + 1, :] = jnp.full((1, w), wp[b] - me * seq, jnp.int32)
        if b >= EARLY:
            continue
        dots = [jnp.sum(of_row(b, j) * of_row(b, 2), axis=-1, keepdims=True) for j in range(2)]
        s = jnp.where(wp[b] < vl[b], jnp.concatenate(dots, axis=0) * scale, -jnp.inf)
        f_ref[b] = jnp.broadcast_to(s, (2 * heads, w))
    for cp in v_copies:
        cp.wait()


def _patch(at_ref, kn_ref, vn_ref, ki_ref, vi_ref, k_ref, v_ref):
    del ki_ref, vi_ref
    rows, seq = k_ref.shape[:2]
    ats = [at_ref[b, 0] for b in range(rows)]
    for b, at in enumerate(ats):
        @pl.when((at >= 0) & (at < seq))
        def _():
            k_ref[b, at] = kn_ref[b]
            v_ref[b, at] = vn_ref[b]


def _attend(n, s_ref, f_ref, q_ref, end_ref, at_ref, k_ref, v_ref, wo_ref, out_ref, w_ref, p_ref, xs, xr, part, recv, red, gath,
            wsem, x2, x3, x4):
    me = lax.axis_index('sp')
    rows, seq, heads, dim = v_ref.shape
    model = out_ref.shape[1]
    cols = red.shape[1]
    blocks = dim // 128
    ntile = seq // TILE
    w = TILE * heads
    span = xs.shape[0] // heads
    barrier = _greet(me, n)
    wcopy = pltpu.make_async_copy(wo_ref, w_ref.at[:, pl.ds(0, model)], wsem)
    wcopy.start()
    w_ref[:, model:] = jnp.zeros((w_ref.shape[0], n * cols - model), BF16)
    lane = lax.broadcasted_iota(jnp.int32, (heads, 128), 1)
    colpos = _positions(heads, w, 2 * seq * n)
    scale = dim ** -0.5

    stats = [jnp.zeros((heads, 128), F32)]
    own_lane = lax.broadcasted_iota(jnp.int32, (rows, 128), 1) - 4 * lax.broadcasted_iota(jnp.int32, (rows, 128), 0)

    def soften(b):
        if b < EARLY:
            at = at_ref[b:b + 1, :]
            fresh = f_ref[b]
            ss = [jnp.where(colpos == at - t * TILE, fresh, s_ref[b, :, t * w:(t + 1) * w]) for t in range(ntile)]
        else:
            end = end_ref[b:b + 1, :]
            ss = [lax.dot_general(q_ref[b], k_ref[b, pl.ds(t * TILE, TILE)].reshape(w, dim), (((1,), (1,)), ((), ())),
                                  preferred_element_type=F32) * scale for t in range(ntile)]
            ss = [jnp.where(colpos < end - t * TILE, s, -jnp.inf) for t, s in enumerate(ss)]
        m = jnp.max(functools.reduce(jnp.maximum, ss), axis=-1, keepdims=True)
        m = jnp.maximum(m, FLOOR)
        ps = [jnp.exp(s - m) for s in ss]
        l = jnp.sum(functools.reduce(jnp.add, ps), axis=-1, keepdims=True)
        for t in range(ntile):
            p_ref[b, :, t * w:(t + 1) * w] = ps[t].astype(BF16)
        here = (lane // 4) == b
        part = [m[:heads], l[:heads], m[heads:], l[heads:]]
        for i, x in enumerate(part):
            stats[0] = jnp.where(here & (lane % 4 == i), x, stats[0])

    def values(b):
        acc = functools.reduce(jnp.add, [
            functools.reduce(jnp.add, [
                jnp.dot(p_ref[b, :, t * w:(t + 1) * w], v_ref[b, pl.ds(t * TILE, TILE)].reshape(w, dim),
                        preferred_element_type=F32) for t in range(first, ntile, 2)]) for first in range(2)])
        for c in range(blocks):
            piece = acc[:, c * 128:(c + 1) * 128]
            xs[pl.ds(c * 2 * rows + b, heads, stride=span), :] = piece[:heads]
            xs[pl.ds(c * 2 * rows + rows + b, heads, stride=span), :] = piece[heads:]

    turn = list(range(EARLY, rows)) + list(range(EARLY))
    for i in range(rows + LAG):
        if i < rows:
            soften(turn[i])
        if i >= LAG:
            values(turn[i - LAG])
    base = blocks * 2 * rows
    xs[pl.ds(base, heads, stride=span), :] = stats[0]
    pl.semaphore_wait(barrier, n - 1)
    _exchange(me, n, lambda peer: xs.at[pl.ds(pl.multiple_of(peer * span, span), base + 1)],
              lambda off: xr.at[off - 1, pl.ds(0, base + 1)], x2)
    xr[n - 1] = xs[_rows(me, span), :]
    _settle(xr.at[pl.ds(0, n - 1), pl.ds(0, base + 1)], x2)
    pieces = []
    def column(i, k):
        return jnp.sum(jnp.where(own_lane == k, xr[i, base:base + 1, :], 0.0), axis=-1, keepdims=True)

    for j in range(2):
        ms = [column(i, 2 * j) for i in range(n)]
        top = functools.reduce(jnp.maximum, ms)
        es = [jnp.exp(m - top) for m in ms]
        total = functools.reduce(jnp.add, [column(i, 2 * j + 1) * es[i] for i in range(n)])
        for c in range(blocks):
            at = c * 2 * rows + j * rows
            num = functools.reduce(jnp.add, [xr[i, at:at + rows, :] * es[i] for i in range(n)])
            pieces.append((num / total).astype(BF16))
    o = jnp.concatenate(pieces, axis=1)
    wcopy.wait()

    order = _far_first(n)
    for group in GROUPS:
        for i in group:
            off = order[i]
            part[off - 1] = jnp.dot(o, w_ref[:, _rows(_peer(me, off, n), cols)], preferred_element_type=F32)
        for i in group:
            off = order[i]
            _send(me, n, off, lambda peer: part.at[off - 1], lambda off: recv.at[off - 1], x3)
    part[n - 1] = jnp.dot(o, w_ref[:, _rows(me, cols)], preferred_element_type=F32)
    _settle(recv, x3)
    total = part[n - 1]
    for off in range(1, n):
        total += recv[off - 1]
    red[...] = total.astype(BF16)
    _exchange(me, n, lambda peer: red, lambda off: gath.at[:, _rows(me, cols)], x4)
    _settle(gath.at[:, pl.ds(0, (n - 1) * cols)], x4)
    gath[:, _rows(me, cols)] = red[...]
    out_ref[...] = gath[:, :model]


def _hand_over(attn_ref, k_ref, v_ref, out_ref):
    del k_ref, v_ref
    out_ref[...] = attn_ref[...]


def solution(mesh):
    row_spec = P(('rep', 'dp'), None)
    cache_spec = P(('rep', 'dp'), 'sp', None, None)
    len_spec = P(('rep', 'dp'))
    n = mesh.shape['sp']
    vmem = pl.BlockSpec(memory_space=pltpu.VMEM)
    hbm = pl.BlockSpec(memory_space=pltpu.HBM)
    dma = pltpu.SemaphoreType.DMA

    def in_hbm(x):
        return pltpu.with_memory_space_constraint(x, pltpu.HBM)

    def local_step(hidden, w_query, w_key, w_value, w_out, k_cache, v_cache, write_pos, valid_len):
        rows, seq, heads, dim = k_cache.shape
        depth = hidden.shape[1]
        model = w_out.shape[1]
        qw = w_query.shape[1] // n
        lw = qw + 2 * dim
        blocks = dim // 128
        cache = pltpu.VMEM(k_cache.shape, BF16)
        new = pltpu.VMEM((rows, heads, dim), BF16)
        scores, fresh, query, ends, at, k_new, v_new, k_here, v_here = pl.pallas_call(
            functools.partial(_project, n),
            out_shape=(
                pltpu.VMEM((EARLY, 2 * heads, seq * heads), F32),
                pltpu.VMEM((EARLY, 2 * heads, TILE * heads), F32),
                pltpu.VMEM((rows, 2 * heads, dim), BF16),
                pltpu.VMEM((rows, TILE * heads), jnp.int32),
                pltpu.VMEM((rows, TILE * heads), jnp.int32),
                new, new, cache, cache,
            ),
            in_specs=[hbm] * 8,
            out_specs=(vmem,) * 9,
            scratch_shapes=[
                pltpu.VMEM((rows, depth), BF16),
                pltpu.VMEM((depth, qw), BF16),
                pltpu.VMEM((depth, dim), BF16),
                pltpu.VMEM((depth, dim), BF16),
                pltpu.VMEM((rows, lw), F32),
                pltpu.VMEM((2, rows, lw // 2), BF16),
                pltpu.VMEM((2, n - 1, rows, lw // 2), BF16),
                pltpu.VMEM((lw // 128, n * rows, 128), F32),
                pltpu.SMEM((rows,), jnp.int32),
                pltpu.SMEM((rows,), jnp.int32),
                dma, dma((len(Q_PARTS),)), dma((2, len(KV_PARTS))), dma((K_PARTS,)), dma((V_PARTS,)), dma((2,)),
                dma((2,)), dma((2,)),
            ],
            compiler_params=pltpu.CompilerParams(collective_id=0, has_side_effects=True, vmem_limit_bytes=12 * MIB),
            cost_estimate=pl.CostEstimate(flops=10_000_000_000, bytes_accessed=28 * MIB, transcendentals=0),
            name='project',
        )(*[in_hbm(x) for x in (hidden, w_query, w_key, w_value, k_cache, v_cache, write_pos, valid_len)])
        k_here, v_here = pl.pallas_call(
            _patch,
            out_shape=(cache, cache),
            in_specs=[vmem] * 5,
            out_specs=(vmem, vmem),
            input_output_aliases={3: 0, 4: 1},
            compiler_params=pltpu.CompilerParams(vmem_limit_bytes=1 * MIB),
            name='patch',
        )(at, k_new, v_new, k_here, v_here)
        top = lax.optimization_barrier(jnp.full((), jnp.inf, BF16))
        k_next = jnp.minimum(k_here, top)
        v_next = jnp.minimum(v_here, top)
        padded = -(-model // (128 * n)) * 128 * n
        span = 2 * rows * blocks + rows
        attn = pl.pallas_call(
            functools.partial(_attend, n),
            out_shape=jax.ShapeDtypeStruct((rows, model), BF16),
            in_specs=[vmem] * 7 + [hbm],
            out_specs=vmem,
            scratch_shapes=[
                pltpu.VMEM((w_out.shape[0], padded), BF16),
                pltpu.VMEM((rows, 2 * heads, seq * heads), BF16),
                pltpu.VMEM((heads * span, 128), F32),
                pltpu.VMEM((n, span, 128), F32),
                pltpu.VMEM((n, rows, padded // n), F32),
                pltpu.VMEM((n - 1, rows, padded // n), F32),
                pltpu.VMEM((rows, padded // n), BF16),
                pltpu.VMEM((rows, padded), BF16),
                dma, dma((2,)), dma((2,)), dma((2,)),
            ],
            compiler_params=pltpu.CompilerParams(collective_id=1, has_side_effects=True, vmem_limit_bytes=8 * MIB),
            cost_estimate=pl.CostEstimate(flops=20_000_000_000, bytes_accessed=4 * MIB, transcendentals=0),
            name='attend',
        )(scores, fresh, query, ends, at, k_next, v_next, in_hbm(w_out))
        attn = pl.pallas_call(
            _hand_over,
            out_shape=jax.ShapeDtypeStruct((rows, model), BF16),
            in_specs=[vmem] * 3,
            out_specs=vmem,
            compiler_params=pltpu.CompilerParams(vmem_limit_bytes=1 * MIB),
            name='hand_over',
        )(attn, k_next, v_next)
        return attn, k_next, v_next

    return jax.shard_map(
        local_step, mesh=mesh,
        in_specs=(row_spec, P(), P(), P(), P('sp', None), cache_spec, cache_spec, len_spec, len_spec),
        out_specs=(row_spec, cache_spec, cache_spec), check_vma=False)
```
